32 devices in a mesh: grp: 2 (over y), row: 16 (over z, x, core).
Axes of the slice: x: 2, y: 2, z: 4, core: 2. Of those that a mesh axis runs over, the one named last changes fastest.
Arguments:
- right_side: float32 [64, 4096], P(None, ('grp', 'row')), may hold values from -60 to 60
- links: int32 [8, 4096], P(None, ('grp', 'row')), may hold values from 0 to 4095, as said below
- coefs: float32 [4096], P(('grp', 'row')), may hold values from 0.3 to 3
- reaction: float32 [4096], P(('grp', 'row')), may hold values from 0.05 to 0.5
Outputs:
- solution: float32 [64, 4096], P(None, ('grp', 'row'))
- resid_rms: float32 [2, 64], replicated
The draws below stay inside these ranges and needn't reach their ends.
Inputs may be any that keep to these rules, and one draw needn't show every extreme that they name: `links`: the nodes form a periodic grid of 8 x 32 x 16. Block (p, q), p < 2, q < 16, holds the nodes of first coordinate p * 4 to p * 4 + 3 and second coordinate q * 2 to q * 2 + 1, and these carry the unknowns and elements b * 4 * 2 * 16 to (b + 1) * 4 * 2 * 16 - 1, with b = p * 16 + q. Element b * 4 * 2 * 16 + (i * 2 + j) * 16 + k has its base at the node (p * 4 + i, q * 2 + j, k), and its corner l lies at the base plus (l mod 2, l // 2 mod 2, l // 4), modulo the grid. Within a block the unknowns are numbered in some order. Every unknown is a corner of 8 elements.
All inputs are finite; a program needn't handle non-finite values.
Results may differ from the reference program's by a relative error of at most 0.0003.
Values sent between devices are 32-bit elements; how exact they have to be, the bound alone decides.
A program may use at most 64 MiB of HBM per device.

```python
import math
import jax
import jax.numpy as jnp
import numpy as np
from jax import lax

CX = 4
CY = 2
CZ = 16
NRHS = 64
SWEEPS = 2
DEGREE = 4
NX = 8
NY = 32
NDOF = 4096
ELEMS = 4096


def draw_right_side(key, part):
    key_noise = jax.random.fold_in(key, 11)
    block_size = CX * CY * CZ
    block_count = NDOF // block_size
    position = (jnp.arange(NDOF) // block_size).astype(jnp.float32)
    rising = 1.0 + 2.0 * position / max(block_count - 1, 1)
    noise = jnp.clip(jax.random.normal(key_noise, (NRHS, NDOF), jnp.float32), -5.0, 5.0)
    return noise * rising


def draw_links(key, part):
    block_size = CX * CY * CZ
    block_count = NDOF // block_size
    row_blocks = NY // CY
    block_keys = jax.vmap(lambda number: jax.random.fold_in(key, number))(jnp.arange(block_count))
    orders = jax.vmap(lambda subkey: jax.random.permutation(subkey, block_size))(block_keys)
    element = jnp.arange(NDOF)
    owner = element // block_size
    inside = element % block_size
    first_block = owner // row_blocks
    second_block = owner % row_blocks
    first_pos = inside // (CY * CZ)
    second_pos = inside // CZ % CY
    third_pos = inside % CZ
    columns = []
    for corner in range(8):
        first = (first_block * CX + first_pos + corner % 2) % NX
        second = (second_block * CY + second_pos + corner // 2 % 2) % NY
        third = (third_pos + corner // 4) % CZ
        target = first // CX * row_blocks + second // CY
        spot = (first % CX * CY + second % CY) * CZ + third
        columns.append(target * block_size + orders[target, spot])
    return jnp.stack(columns, axis=0).astype(jnp.int32)


def levels(own_key, extent, cuts, least, top_value):
    def one(dim, parts):
        heights = jax.random.uniform(jax.random.fold_in(jax.random.fold_in(own_key, 6), dim), (parts,), jnp.float32, least / len(cuts), top_value / len(cuts))
        return jnp.repeat(jnp.exp(heights), extent[dim] // parts).reshape((-1,) + (1,) * (len(extent) - dim - 1))

    loudness = one(*cuts[0])
    for cut in cuts[1:]:
        loudness = loudness * one(*cut)
    return loudness


def setup_inputs(seed: int = 0) -> dict:
    streams_of = jax.random.split(jax.random.key(seed), 5)
    return {
        "right_side": draw_right_side(jax.random.fold_in(streams_of[4], 71), 0),
        "links": draw_links(jax.random.fold_in(streams_of[4], 71), 0),
        "coefs": jnp.clip(jnp.exp(math.log(3.0) - 2.3025851 * jax.random.uniform(streams_of[2], (ELEMS,), jnp.float32) ** levels(streams_of[2], (ELEMS,), ((0, 32),), -0.2, 0.2)), 0.3, 3.0),
        "reaction": jnp.clip(jnp.exp(math.log(0.5) - 2.3025851 * jax.random.uniform(streams_of[3], (NDOF,), jnp.float32) ** levels(streams_of[3], (NDOF,), ((0, 32),), -0.2, 0.2)), 0.05, 0.5),
    }


def element_matrix():
    node_ids = np.arange(8)
    corner = np.stack([node_ids % 2, node_ids // 2 % 2, node_ids // 4], axis=1)
    gauss_points = np.array([0.5 - 0.5 / math.sqrt(3.0), 0.5 + 0.5 / math.sqrt(3.0)])
    stiffness = np.zeros((8, 8))
    for q in range(8):
        quad_point = gauss_points[np.array([q % 2, q // 2 % 2, q // 4])]
        values = np.where(corner > 0.5, quad_point, 1.0 - quad_point)
        slopes = np.where(corner > 0.5, 1.0, -1.0)
        gradient = np.stack([slopes[:, 0] * values[:, 1] * values[:, 2], values[:, 0] * slopes[:, 1] * values[:, 2], values[:, 0] * values[:, 1] * slopes[:, 2]], axis=1)
        stiffness = stiffness + gradient @ gradient.T / 8.0
    return stiffness

def apply_operator(field, links, coefs, reaction, stiffness):
    corners = field[:, links]
    images = jnp.einsum('ml,rle->rme', stiffness, corners, precision=lax.Precision.HIGHEST) * coefs
    result = reaction * field
    return result.at[:, links].add(images)

def reference(right_side, links, coefs, reaction):
    stiffness = jnp.asarray(element_matrix(), dtype=jnp.float32)
    image = apply_operator(right_side, links, coefs, reaction, stiffness)
    theta = lax.optimization_barrier(jnp.sum(image * image, axis=1)) / lax.optimization_barrier(jnp.sum(right_side * image, axis=1))
    upper = (1.5 * theta)[:, None]
    lower = upper / 10.0
    center = (upper + lower) / 2.0
    half = (upper - lower) / 2.0
    sigma = center / half
    solution = jnp.zeros_like(right_side)
    residual = right_side
    history = []
    for sweep in range(SWEEPS):
        start = residual
        correction = jnp.zeros_like(right_side)
        rho_now = 1.0 / sigma
        direction = residual / center
        for step in range(DEGREE):
            correction = correction + direction
            residual = residual - apply_operator(direction, links, coefs, reaction, stiffness)
            if step + 1 < DEGREE:
                rho_next = 1.0 / (2.0 * sigma - rho_now)
                direction = rho_next * rho_now * direction + 2.0 * rho_next / half * residual
                rho_now = rho_next
        change = start - residual
        omega = (lax.optimization_barrier(jnp.sum(start * change, axis=1)) / lax.optimization_barrier(jnp.sum(change * change, axis=1)))[:, None]
        solution = solution + omega * correction
        residual = start - omega * change
        history.append(jnp.sqrt(lax.optimization_barrier(jnp.sum(residual * residual, axis=1)) / NDOF))
    return (solution, jnp.stack(history, axis=0))
```

```python
import functools
import math

import jax
import jax.numpy as jnp
import numpy as np
from jax import lax
from jax.experimental import pallas as pl
from jax.experimental.pallas import tpu as pltpu
from jax.sharding import PartitionSpec as P

SWEEPS = 2
DEGREE = 4
CX, CY, CZ = 4, 2, 16
SUB, LANES = 8, 128
MESH = pl.DeviceIdType.MESH
HIGHEST = lax.Precision.HIGHEST


def shifted(block, axis, distance):
    devices = range(lax.axis_size(axis))
    route = [((i - distance) % len(devices), i) for i in devices]
    return lax.ppermute(block, axis, route)


def element_matrix():
    node_ids = np.arange(8)
    corner = np.stack([node_ids % 2, node_ids // 2 % 2, node_ids // 4], axis=1)
    gauss_points = np.array([0.5 - 0.5 / math.sqrt(3.0), 0.5 + 0.5 / math.sqrt(3.0)])
    stiffness = np.zeros((8, 8))
    for q in range(8):
        quad_point = gauss_points[np.array([q % 2, q // 2 % 2, q // 4])]
        values = np.where(corner > 0.5, quad_point, 1.0 - quad_point)
        slopes = np.where(corner > 0.5, 1.0, -1.0)
        gradient = np.stack(
            [
                slopes[:, 0] * values[:, 1] * values[:, 2],
                values[:, 0] * slopes[:, 1] * values[:, 2],
                values[:, 0] * values[:, 1] * slopes[:, 2],
            ],
            axis=1,
        )
        stiffness = stiffness + gradient @ gradient.T / 8.0
    return stiffness


def element_images(window, offsets, weights, stiffness):
    corners = window[:, offsets]
    images = (
        jnp.einsum("ml,rle->rme", stiffness, corners, precision=lax.Precision.HIGHEST) * weights
    )
    return jnp.zeros_like(window).at[:, offsets].add(images)


def on_device(right_side, links, coefs, reaction):
    stiffness = jnp.asarray(element_matrix(), dtype=jnp.float32)
    count = right_side.shape[1]
    groups = lax.axis_size("grp")
    rowcount = lax.axis_size("row")
    group_id = lax.axis_index("grp")
    row_id = lax.axis_index("row")
    total = count * groups * rowcount
    owner = links // count
    slot = links % count
    first = jnp.mod(owner // rowcount - group_id, groups)
    second = jnp.mod(owner % rowcount - row_id, rowcount)
    offsets = (first * 2 + second) * count + slot

    def apply_operator(field):
        above_row = shifted(field, "row", -1)
        upper = shifted(jnp.stack([field, above_row], axis=0), "grp", -1)
        window = jnp.concatenate([field, above_row, upper[0], upper[1]], axis=1)
        summed = element_images(window, offsets, coefs, stiffness)
        back = shifted(
            jnp.stack([summed[:, 2 * count : 3 * count], summed[:, 3 * count :]], axis=0), "grp", 1
        )
        first_col = summed[:, :count] + back[0]
        second_col = summed[:, count : 2 * count] + back[1]
        first_col = first_col + shifted(second_col, "row", 1)
        return first_col + reaction * field

    image = apply_operator(right_side)
    cross, square = lax.psum(
        (jnp.sum(right_side * image, axis=1), jnp.sum(image * image, axis=1)), ("grp", "row")
    )
    theta = square / cross
    upper = (1.5 * theta)[:, None]
    lower = upper / 10.0
    center = (upper + lower) / 2.0
    half = (upper - lower) / 2.0
    sigma = center / half
    solution = jnp.zeros_like(right_side)
    residual = right_side
    history = []
    for sweep in range(SWEEPS):
        start = residual
        correction = jnp.zeros_like(right_side)
        rho_now = 1.0 / sigma
        direction = residual / center
        for step in range(DEGREE):
            correction = correction + direction
            residual = residual - apply_operator(direction)
            if step + 1 < DEGREE:
                rho_next = 1.0 / (2.0 * sigma - rho_now)
                direction = rho_next * rho_now * direction + 2.0 * rho_next / half * residual
                rho_now = rho_next
        change = start - residual
        along, length, begin = lax.psum(
            (
                jnp.sum(start * change, axis=1),
                jnp.sum(change * change, axis=1),
                jnp.sum(start * start, axis=1),
            ),
            ("grp", "row"),
        )
        omega = along / length
        residual = start - omega[:, None] * change
        squares = begin - 2.0 * omega * along + omega * omega * length
        solution = solution + omega[:, None] * correction
        history.append(jnp.sqrt(squares / total))
    return (solution, jnp.stack(history, axis=0))


def thirds(a):
    high = a.astype(jnp.bfloat16).astype(jnp.float32)
    rest = a - high
    middle = rest.astype(jnp.bfloat16).astype(jnp.float32)
    return [high, middle, rest - middle]


def added(parts):
    high, middle, low = parts
    return high + middle + low


def turned(a, distance, axis=1):
    return pltpu.roll(a, distance % a.shape[axis], axis)


def chebyshev_steps():
    sigma = (1.5 + 0.15) / (1.5 - 0.15)
    rho_now = 1.0 / sigma
    steps = []
    for _ in range(DEGREE - 1):
        rho_next = 1.0 / (2.0 * sigma - rho_now)
        steps.append((rho_next * rho_now, 2.0 * rho_next / ((1.5 - 0.15) / 2.0)))
        rho_now = rho_next
    return 2.0 / (1.5 + 0.15), steps


def kernel(
    groups, rowcount, total,
    right_ref, links_ref, coefs_ref, react_ref,
    packed_ref,
    outbox, inbox, answers, solved, weights, order,
    bases, changes, directions, corrections, residuals, settled,
    out_send, out_recv, back_send, back_recv,
):
    nrhs, count = right_ref.shape
    leaders = nrhs // SUB
    heads = leaders // groups
    blocks = groups * rowcount
    half_lane = CX
    z_lane = CX * CY
    grp = lax.axis_index("grp")
    row = lax.axis_index("row")
    me = grp * rowcount + row
    leading = row < heads
    rank = grp * heads + row

    def leader(t):
        return (t // heads, lax.rem(t, heads))

    def block(b):
        return (b // rowcount, lax.rem(b, rowcount))

    def place_of(t):
        return (t // heads) * rowcount + lax.rem(t, heads)

    barrier = pltpu.get_barrier_semaphore()

    @pl.when(leading)
    def _():
        for o in range(1, blocks):
            pl.semaphore_signal(
                barrier, inc=1, device_id=block(lax.rem(me + o, blocks)), device_id_type=MESH
            )

    lane = lax.broadcasted_iota(jnp.int32, (count, count), 1)
    down = lax.broadcasted_iota(jnp.int32, (count, count), 0)
    element = ((lane % CX) * CY + lane // CX % CY) * CZ + lane // z_lane
    to_lanes = (down == element).astype(jnp.float32)
    slots = (links_ref[0:1, :] - me * count).astype(jnp.float32)
    mass = thirds(coefs_ref[...] * (1.0 / 12.0))
    small = jnp.concatenate([slots] + mass + [jnp.zeros((SUB - 4, count), jnp.float32)], axis=0)
    small = jnp.dot(small, to_lanes, preferred_element_type=jnp.float32)
    mass = added([small[k : k + 1] for k in (1, 2, 3)])
    order[...] = (down.astype(jnp.float32) == small[0:1]).astype(jnp.float32)
    react = thirds(react_ref[...])
    react = jnp.concatenate(react + [jnp.zeros((SUB - 3, count), jnp.float32)], axis=0)
    stack = jnp.concatenate(thirds(right_ref[...]) + [react], axis=0)
    stack = jnp.dot(stack, order[...], preferred_element_type=jnp.float32)
    field = added([stack[k * nrhs : (k + 1) * nrhs] for k in range(3)])
    react = added([stack[3 * nrhs + k : 3 * nrhs + k + 1] for k in range(3)])
    extra = jnp.concatenate([mass, react], axis=0)
    for t in range(leaders):
        outbox[t, 0:SUB] = field[t * SUB : (t + 1) * SUB]
        outbox[t, SUB : SUB + 2] = extra

    pl.semaphore_wait(barrier, jnp.where(leading, leaders - 1, leaders))

    def post(o):
        t = lax.rem(rank + o, leaders)
        return pltpu.make_async_remote_copy(
            src_ref=outbox.at[t], dst_ref=inbox.at[me],
            send_sem=out_send.at[t], recv_sem=out_recv.at[me],
            device_id=leader(t), device_id_type=MESH,
        )

    for o in range(1, leaders):
        post(o).start()

    @pl.when(jnp.logical_not(leading))
    def _():
        post(0).start()

    def reply(b):
        return pltpu.make_async_remote_copy(
            src_ref=solved.at[b], dst_ref=answers.at[rank],
            send_sem=back_send.at[b], recv_sem=back_recv.at[rank],
            device_id=block(b), device_id_type=MESH,
        )

    @pl.when(leading)
    def _():
        inbox[me] = outbox[rank]
        for o in range(1, blocks):
            b = lax.rem(me + o, blocks)
            pltpu.make_async_remote_copy(
                src_ref=outbox.at[0], dst_ref=inbox.at[b],
                send_sem=out_send.at[0], recv_sem=out_recv.at[b],
                device_id=block(b), device_id_type=MESH,
            ).wait_recv()

        rows_lane = lax.broadcasted_iota(jnp.int32, (rowcount, count), 1)
        in_second = rows_lane // CX % CY == 1
        in_first = rows_lane % CX > 0
        plus, minus = [], []
        for p in range(groups):
            m = inbox[p * rowcount : (p + 1) * rowcount, SUB, :]
            up4, up12 = turned(m, half_lane), turned(m, half_lane + z_lane)
            down4 = turned(m, -half_lane)
            plus.append([
                m,
                turned(m, z_lane),
                jnp.where(in_second, up4, turned(down4, 1, 0)),
                jnp.where(in_second, up12, turned(up4, 1, 0)),
            ])
        for p in range(groups):
            before = plus[(p - 1) % groups]
            minus.append([
                jnp.where(in_first, turned(m, 1), turned(other, 1 - CX))
                for m, other in zip(plus[p], before)
            ])
        for p in range(groups):
            rows = slice(p * rowcount, (p + 1) * rowcount)
            both = [-(a + b) for a, b in zip(plus[p], minus[p])]
            diag = inbox[rows, SUB + 1, :] - 4.0 * (both[0] + both[1] + both[2] + both[3])
            for k in range(4):
                weights[k, rows] = -minus[p][k]
                weights[4 + k, rows] = -plus[p][k]
                weights[8 + k, rows] = both[k]
            weights[12, rows] = diag

        tile_lane = lax.broadcasted_iota(jnp.int32, (SUB, count), 1)
        is_second = tile_lane // CX % CY == 1
        first_low = tile_lane % CX == 0
        first_top = tile_lane % CX == CX - 1

        def apply_operator(source, sink):
            rolled = {}

            def rolls(p, q):
                q = q % rowcount
                if (p, q) not in rolled:
                    v = source(p * rowcount + q)
                    near = half_lane
                    rolled[p, q] = (
                        v, turned(v, -z_lane), turned(v, z_lane),
                        turned(v, near), turned(v, -near),
                        turned(v, near + z_lane), turned(v, -near - z_lane),
                    )
                return rolled[p, q]

            for q in range(rowcount):
                forward, backward, middle = [], [], []
                for p in range(groups):
                    b = p * rowcount + q
                    v, above, below, up4, down4, up12, down12 = rolls(p, q)
                    _, _, _, next4, nextd4, next12, _ = rolls(p, q + 1)
                    _, _, _, last4, lastd4, _, lastd12 = rolls(p, q - 1)
                    near = jnp.where(is_second, next4, down4)
                    far = jnp.where(is_second, up4, lastd4)
                    diagonal = [
                        jnp.where(is_second, nextd4, down12),
                        jnp.where(is_second, next12, up4),
                        jnp.where(is_second, down4, lastd12),
                        jnp.where(is_second, up12, last4),
                    ]
                    sides = [
                        above + (near + diagonal[0]),
                        below + (near + diagonal[1]),
                        above + (far + diagonal[2]),
                        below + (far + diagonal[3]),
                    ]
                    w = [weights[k, b : b + 1, :] for k in range(13)]
                    forward.append(
                        (w[0] * sides[0] + w[1] * sides[1]) + (w[2] * sides[2] + w[3] * sides[3])
                    )
                    backward.append(
                        (w[4] * sides[0] + w[5] * sides[1]) + (w[6] * sides[2] + w[7] * sides[3])
                    )
                    middle.append(
                        (w[8] * diagonal[0] + w[9] * diagonal[1])
                        + (w[10] * diagonal[2] + w[11] * diagonal[3])
                        + w[12] * v
                    )
                for p in range(groups):
                    after, before = (p + 1) % groups, (p - 1) % groups
                    ahead = jnp.where(first_top, turned(forward[after], CX - 1), turned(forward[p], -1))
                    behind = jnp.where(
                        first_low, turned(backward[before], 1 - CX), turned(backward[p], 1)
                    )
                    sink(p * rowcount + q, middle[p] + (ahead + behind))

        def across(parts):
            total_ = (parts[0] + parts[1]) + (parts[2] + parts[3])
            return jnp.broadcast_to(jnp.sum(total_, axis=1, keepdims=True), (SUB, count))

        class Sum:
            def __init__(self):
                self.parts = [None] * 4
                self.at = 0

            def add(self, value):
                k = self.at % 4
                self.parts[k] = value if self.parts[k] is None else self.parts[k] + value
                self.at += 1

            def get(self):
                return across(self.parts)

        scale, steps = chebyshev_steps()
        square, cross = Sum(), Sum()

        def first_image(b, image):
            start = inbox[b, 0:SUB]
            residuals[b] = image
            square.add(image * image)
            cross.add(start * image)

        apply_operator(lambda b: inbox[b, 0:SUB], first_image)
        inverse = cross.get() / square.get()
        opening = scale * inverse

        first_rms = second_rms = None
        omegas = []
        for sweep in range(SWEEPS):
            along, length, begin = Sum(), Sum(), Sum()
            start_of = (lambda b: inbox[b, 0:SUB]) if sweep == 0 else (lambda b: bases[b])
            for step in range(DEGREE):
                here, there = directions.at[step % 2], directions.at[(step + 1) % 2]

                def finish(b, image, step=step, here=here, there=there, sweep=sweep):
                    before = start_of(b) if step == 0 else residuals[b]
                    direction = here[b]
                    residual = before - image
                    if step + 1 < DEGREE:
                        keep, gain = steps[step]
                        following = keep * direction + (gain * inverse) * residual
                        residuals[b] = residual
                        there[b] = following
                        so_far = direction if step == 0 else corrections[sweep, b]
                        corrections[sweep, b] = so_far + following
                    else:
                        start = start_of(b)
                        change = start - residual
                        changes[b] = change
                        along.add(start * change)
                        length.add(change * change)

                if sweep == 0 and step == 0:
                    for b in range(blocks):
                        here[b] = opening * inbox[b, 0:SUB]
                        finish(b, opening * residuals[b])
                else:
                    apply_operator(lambda b, here=here: here[b], finish)
            omega = along.get() / length.get()
            omegas.append(omega)
            if sweep + 1 < SWEEPS:
                for b in range(blocks):
                    base = start_of(b) - omega * changes[b]
                    bases[b] = base
                    directions[0, b] = opening * base
                    begin.add(base * base)
                began = begin.get()
            else:
                squares = jnp.maximum(began - omega * along.get(), 0.0)
        sweeps = [jnp.sqrt(began / total), jnp.sqrt(squares / total)]
        which = lax.broadcasted_iota(jnp.int32, (SUB, count), 0) + rank * SUB
        rms = jnp.where(tile_lane == which, sweeps[0], 0.0)
        rms = jnp.where(tile_lane == which + count // 2, sweeps[1], rms)
        rms = jnp.sum(rms, axis=0, keepdims=True)
        for b in range(blocks):
            solved[b, 0:SUB] = omegas[0] * corrections[0, b] + omegas[1] * corrections[1, b]
            solved[b, SUB : SUB + 1] = rms
        for o in range(1, leaders):
            reply(place_of(lax.rem(rank + o, leaders))).start()
        for g in range(groups):
            for r in range(heads, rowcount):
                reply(g * rowcount + r).start()
        answers[rank] = solved[me]

    def await_reply(t):
        pltpu.make_async_remote_copy(
            src_ref=solved.at[0], dst_ref=answers.at[t],
            send_sem=back_send.at[0], recv_sem=back_recv.at[t],
            device_id=leader(t), device_id_type=MESH,
        ).wait_recv()

    for o in range(1, leaders):
        await_reply(lax.rem(rank + o, leaders))

    @pl.when(jnp.logical_not(leading))
    def _():
        await_reply(lax.rem(rank, leaders))

    whole = jnp.concatenate([answers[t, 0:SUB] for t in range(leaders)], axis=0)
    whole = jnp.concatenate(thirds(whole), axis=0)
    whole = lax.dot_general(
        whole, order[...], (((1,), (1,)), ((), ())), preferred_element_type=jnp.float32
    )
    packed_ref[0:nrhs] = added([whole[k * nrhs : (k + 1) * nrhs] for k in range(3)])
    line = answers[0, SUB : SUB + 1]
    for t in range(1, leaders):
        line = line + answers[t, SUB : SUB + 1]
    packed_ref[nrhs : nrhs + SUB] = jnp.concatenate(
        [line, turned(line, count // 2), jnp.zeros((SUB - 2, count), jnp.float32)], axis=0
    )

    for o in range(1, leaders):
        post(o).wait_send()

    @pl.when(jnp.logical_not(leading))
    def _():
        post(0).wait_send()

    @pl.when(leading)
    def _():
        for o in range(1, blocks):
            reply(lax.rem(me + o, blocks)).wait_send()


def unpack(packed_ref, out_ref, rms_ref):
    nrhs = out_ref.shape[0]
    out_ref[...] = packed_ref[:nrhs]
    rms_ref[...] = packed_ref[nrhs : nrhs + SWEEPS, :nrhs]


def whole_sweeps(groups, rowcount, right_side, links, coefs, reaction):
    nrhs, count = right_side.shape
    leaders = nrhs // SUB
    blocks = groups * rowcount
    dma = pltpu.SemaphoreType.DMA
    vmem = pl.BlockSpec(memory_space=pltpu.VMEM)

    def space(*shape):
        return pltpu.VMEM(shape, jnp.float32)

    packed = pl.pallas_call(
        functools.partial(kernel, groups, rowcount, count * groups * rowcount),
        out_shape=jax.ShapeDtypeStruct((nrhs + SUB, count), jnp.float32),
        in_specs=[vmem] * 4,
        out_specs=vmem,
        scratch_shapes=[
            space(leaders, SUB + 2, count), space(blocks, SUB + 2, count),
            space(leaders, SUB + 1, count), space(blocks, SUB + 1, count),
            space(13, blocks, count), space(count, count),
            space(blocks, SUB, count), space(blocks, SUB, count), space(2, blocks, SUB, count),
            space(SWEEPS, blocks, SUB, count), space(blocks, SUB, count), space(SUB, count),
            dma((leaders,)), dma((blocks,)), dma((blocks,)), dma((leaders,)),
        ],
        compiler_params=pltpu.CompilerParams(collective_id=0, has_side_effects=True),
    )(right_side, links, coefs.reshape(1, count), reaction.reshape(1, count))
    return pl.pallas_call(
        unpack,
        out_shape=(
            jax.ShapeDtypeStruct((nrhs, count), jnp.float32),
            jax.ShapeDtypeStruct((SWEEPS, nrhs), jnp.float32),
        ),
        in_specs=[vmem],
        out_specs=(vmem, vmem),
    )(packed)


def in_one_kernel(mesh):
    return mesh.shape["grp"] == 2 and 2 * SUB <= mesh.shape["row"] <= 4 * SUB


def solution(mesh):
    body = on_device
    if in_one_kernel(mesh):
        body = functools.partial(whole_sweeps, mesh.shape["grp"], mesh.shape["row"])
    return jax.shard_map(
        body,
        mesh=mesh,
        in_specs=(
            P(None, ("grp", "row")),
            P(None, ("grp", "row")),
            P(("grp", "row")),
            P(("grp", "row")),
        ),
        out_specs=(P(None, ("grp", "row")), P()),
        check_vma=False,
    )
```

```python
import functools
import math

import jax
import jax.numpy as jnp
import numpy as np
from jax import lax
from jax.experimental import pallas as pl
from jax.experimental.pallas import tpu as pltpu
from jax.sharding import PartitionSpec as P

SWEEPS = 2
DEGREE = 4
CX, CY, CZ = 4, 2, 16
SUB, LANES = 8, 128
MESH = pl.DeviceIdType.MESH
HIGHEST = lax.Precision.HIGHEST


def shifted(block, axis, distance):
    devices = range(lax.axis_size(axis))
    route = [((i - distance) % len(devices), i) for i in devices]
    return lax.ppermute(block, axis, route)


def element_matrix():
    node_ids = np.arange(8)
    corner = np.stack([node_ids % 2, node_ids // 2 % 2, node_ids // 4], axis=1)
    gauss_points = np.array([0.5 - 0.5 / math.sqrt(3.0), 0.5 + 0.5 / math.sqrt(3.0)])
    stiffness = np.zeros((8, 8))
    for q in range(8):
        quad_point = gauss_points[np.array([q % 2, q // 2 % 2, q // 4])]
        values = np.where(corner > 0.5, quad_point, 1.0 - quad_point)
        slopes = np.where(corner > 0.5, 1.0, -1.0)
        gradient = np.stack(
            [
                slopes[:, 0] * values[:, 1] * values[:, 2],
                values[:, 0] * slopes[:, 1] * values[:, 2],
                values[:, 0] * values[:, 1] * slopes[:, 2],
            ],
            axis=1,
        )
        stiffness = stiffness + gradient @ gradient.T / 8.0
    return stiffness


def element_images(window, offsets, weights, stiffness):
    corners = window[:, offsets]
    images = (
        jnp.einsum("ml,rle->rme", stiffness, corners, precision=lax.Precision.HIGHEST) * weights
    )
    return jnp.zeros_like(window).at[:, offsets].add(images)


def on_device(right_side, links, coefs, reaction):
    stiffness = jnp.asarray(element_matrix(), dtype=jnp.float32)
    count = right_side.shape[1]
    groups = lax.axis_size("grp")
    rowcount = lax.axis_size("row")
    group_id = lax.axis_index("grp")
    row_id = lax.axis_index("row")
    total = count * groups * rowcount
    owner = links // count
    slot = links % count
    first = jnp.mod(owner // rowcount - group_id, groups)
    second = jnp.mod(owner % rowcount - row_id, rowcount)
    offsets = (first * 2 + second) * count + slot

    def apply_operator(field):
        above_row = shifted(field, "row", -1)
        upper = shifted(jnp.stack([field, above_row], axis=0), "grp", -1)
        window = jnp.concatenate([field, above_row, upper[0], upper[1]], axis=1)
        summed = element_images(window, offsets, coefs, stiffness)
        back = shifted(
            jnp.stack([summed[:, 2 * count : 3 * count], summed[:, 3 * count :]], axis=0), "grp", 1
        )
        first_col = summed[:, :count] + back[0]
        second_col = summed[:, count : 2 * count] + back[1]
        first_col = first_col + shifted(second_col, "row", 1)
        return first_col + reaction * field

    image = apply_operator(right_side)
    cross, square = lax.psum(
        (jnp.sum(right_side * image, axis=1), jnp.sum(image * image, axis=1)), ("grp", "row")
    )
    theta = square / cross
    upper = (1.5 * theta)[:, None]
    lower = upper / 10.0
    center = (upper + lower) / 2.0
    half = (upper - lower) / 2.0
    sigma = center / half
    solution = jnp.zeros_like(right_side)
    residual = right_side
    history = []
    for sweep in range(SWEEPS):
        start = residual
        correction = jnp.zeros_like(right_side)
        rho_now = 1.0 / sigma
        direction = residual / center
        for step in range(DEGREE):
            correction = correction + direction
            residual = residual - apply_operator(direction)
            if step + 1 < DEGREE:
                rho_next = 1.0 / (2.0 * sigma - rho_now)
                direction = rho_next * rho_now * direction + 2.0 * rho_next / half * residual
                rho_now = rho_next
        change = start - residual
        along, length, begin = lax.psum(
            (
                jnp.sum(start * change, axis=1),
                jnp.sum(change * change, axis=1),
                jnp.sum(start * start, axis=1),
            ),
            ("grp", "row"),
        )
        omega = along / length
        residual = start - omega[:, None] * change
        squares = begin - 2.0 * omega * along + omega * omega * length
        solution = solution + omega[:, None] * correction
        history.append(jnp.sqrt(squares / total))
    return (solution, jnp.stack(history, axis=0))


def thirds(a):
    high = a.astype(jnp.bfloat16).astype(jnp.float32)
    rest = a - high
    middle = rest.astype(jnp.bfloat16).astype(jnp.float32)
    return [high, middle, rest - middle]


def added(parts):
    high, middle, low = parts
    return high + middle + low


def turned(a, distance, axis=1):
    return pltpu.roll(a, distance % a.shape[axis], axis)


def tile_iota(axis):
    return lax.broadcasted_iota(jnp.int32, (SUB, LANES), axis)


def exchanged(tile):
    sub, low = tile_iota(0), tile_iota(1)
    for bit in (1, 2, 4):
        rise = turned(turned(tile, -bit, 0), bit)
        fall = turned(turned(tile, bit, 0), -bit)
        in_low, in_sub = low // bit % 2, sub // bit % 2
        tile = jnp.where(in_low > in_sub, rise, jnp.where(in_low < in_sub, fall, tile))
    return tile


def paired(first, second):
    top = tile_iota(0) < SUB // 2
    return (
        jnp.where(top, first, turned(second, SUB // 2, 0)),
        jnp.where(top, turned(first, SUB // 2, 0), second),
    )


def chebyshev_steps():
    sigma = (1.5 + 0.15) / (1.5 - 0.15)
    rho_now = 1.0 / sigma
    steps = []
    for _ in range(DEGREE - 1):
        rho_next = 1.0 / (2.0 * sigma - rho_now)
        steps.append((rho_next * rho_now, 2.0 * rho_next / ((1.5 - 0.15) / 2.0)))
        rho_now = rho_next
    return 2.0 / (1.5 + 0.15), steps


class Total:
    def __init__(self):
        self.parts = [None] * 4
        self.at = 0

    def add(self, value):
        k = self.at % 4
        self.parts[k] = value if self.parts[k] is None else self.parts[k] + value
        self.at += 1

    def folded(self):
        a, b, c, d = self.parts
        value = (a + b) + (c + d)
        for bit in (4, 2, 1):
            value = value + turned(value, bit, 0)
        return value


def over_z(value):
    parts = [value] + [turned(value, SUB * k) for k in range(1, LANES // SUB)]
    while len(parts) > 1:
        parts = [a + b for a, b in zip(parts[::2], parts[1::2])]
    return parts[0]


def summed(first, second):
    top = tile_iota(0) < SUB // 2
    both = over_z(jnp.where(top, first.folded(), second.folded()))
    other = turned(both, SUB // 2, 0)
    return jnp.where(top, both, other), jnp.where(top, other, both)


def kernel(
    groups, rowcount, total,
    right_hbm, links_hbm, coefs_hbm, react_hbm,
    packed_ref,
    right_ref, links_ref, coefs_ref, react_ref,
    auxout, auxin, outbox, inbox, answers, solved, order, spread, wide,
    masses, masses_z, lows, lows_z, boths, boths_z, diag,
    bases, changes, directions, corrections, residuals,
    in_sem, aux_send, aux_recv, out_send, out_recv, back_send, back_recv,
):
    nrhs, count = right_ref.shape
    leaders = nrhs // SUB
    heads = leaders // groups
    blocks = groups * rowcount
    planes = rowcount * CY
    grp = lax.axis_index("grp")
    row = lax.axis_index("row")
    me = grp * rowcount + row
    leading = row < heads
    rank = grp * heads + row

    def leader(t):
        return (t // heads, lax.rem(t, heads))

    def block(b):
        return (b // rowcount, lax.rem(b, rowcount))

    def place_of(t):
        return (t // heads) * rowcount + lax.rem(t, heads)

    barrier = pltpu.get_barrier_semaphore()

    @pl.when(leading)
    def _():
        far = sorted(range(1, blocks), key=lambda o: -min(o % rowcount, rowcount - o % rowcount))
        for o in far:
            pl.semaphore_signal(
                barrier, inc=1, device_id=block(lax.rem(me + o, blocks)), device_id_type=MESH
            )

    loads = [
        pltpu.make_async_copy(source, target, in_sem.at[k])
        for k, (source, target) in enumerate(
            [(links_hbm, links_ref), (coefs_hbm, coefs_ref), (react_hbm, react_ref), (right_hbm, right_ref)]
        )
    ]
    for load in loads:
        load.start()

    lane = lax.broadcasted_iota(jnp.int32, (count, count), 1)
    down = lax.broadcasted_iota(jnp.int32, (count, count), 0)
    element = ((lane % CX) * CY + lane // CX % CY) * CZ + lane // SUB
    to_lanes = (down == element).astype(jnp.float32)
    same_z = (down // SUB == lane // SUB).astype(jnp.float32)
    spread[0:count] = same_z
    spread[count : 2 * count] = same_z

    for load in loads[:3]:
        load.wait()
    slots = (links_ref[0:1, :] - me * count).astype(jnp.float32)
    mass = thirds(coefs_ref[...] * (-1.0 / 12.0))
    small = jnp.concatenate([slots] + mass + [jnp.zeros((SUB - 4, count), jnp.float32)], axis=0)
    small = jnp.dot(small, to_lanes, preferred_element_type=jnp.float32)
    mass = added([small[k : k + 1] for k in (1, 2, 3)])
    order[...] = (down.astype(jnp.float32) == small[0:1]).astype(jnp.float32)
    react = thirds(react_ref[...])
    react = jnp.concatenate(react + [jnp.zeros((SUB - 3, count), jnp.float32)], axis=0)
    loads[3].wait()
    stack = jnp.concatenate([react] + thirds(right_ref[...]), axis=0)
    stack = jnp.dot(stack, order[...], preferred_element_type=jnp.float32)
    react = added([stack[k : k + 1] for k in range(3)])
    auxout[...] = jnp.concatenate([mass, react], axis=0)
    field = added([stack[SUB + k * nrhs : SUB + (k + 1) * nrhs] for k in range(3)])

    def post(o, source, target, send, recv):
        t = lax.rem(rank + o, leaders)
        return pltpu.make_async_remote_copy(
            src_ref=source(t), dst_ref=target.at[me], send_sem=send.at[t], recv_sem=recv,
            device_id=leader(t), device_id_type=MESH,
        )

    def post_aux(o):
        return post(o, lambda t: auxout, auxin, aux_send, aux_recv.at[me])

    def post_field(o):
        return post(o, lambda t: outbox.at[t], inbox, out_send, out_recv.at[me])

    for t in range(leaders):
        outbox[t] = exchanged(field[t * SUB : (t + 1) * SUB])
    pl.semaphore_wait(barrier, jnp.where(leading, leaders - 1, leaders))

    for send in (post_aux, post_field):
        for o in range(1, leaders):
            send(o).start()

        @pl.when(jnp.logical_not(leading))
        def _(send=send):
            send(0).start()

    def reply(b):
        return pltpu.make_async_remote_copy(
            src_ref=solved.at[b], dst_ref=answers.at[rank],
            send_sem=back_send.at[b], recv_sem=back_recv.at[rank],
            device_id=block(b), device_id_type=MESH,
        )

    @pl.when(leading)
    def _():
        auxin[me] = auxout[...]
        for o in range(1, blocks):
            b = lax.rem(me + o, blocks)
            pltpu.make_async_remote_copy(
                src_ref=auxout, dst_ref=auxin.at[b],
                send_sem=aux_send.at[0], recv_sem=aux_recv.at[b],
                device_id=block(b), device_id_type=MESH,
            ).wait_recv()

        own = tile_iota(1) % SUB == tile_iota(0)
        for k in range(2):
            high, middle, _ = thirds(auxin[:, k, :])
            wide[0, k * blocks : (k + 1) * blocks] = high
            wide[1, k * blocks : (k + 1) * blocks] = middle
        pieces = [
            jnp.concatenate(
                [jnp.where(own, wide[part, k : k + 1, :], 0.0) for k in range(2 * blocks)], axis=0
            )
            for part in range(2)
        ]
        tiles = jnp.dot(
            jnp.concatenate(pieces, axis=1), spread[...], preferred_element_type=jnp.float32
        )
        tiles = [tiles[k * SUB : (k + 1) * SUB] for k in range(2 * blocks)]
        for q in range(rowcount):
            for k, m in enumerate(paired(tiles[q], tiles[rowcount + q])):
                y = CY * q + k
                m_z = turned(m, SUB)
                low, low_z = turned(m, 1, 0), turned(m_z, 1, 0)
                masses[y], masses_z[y] = m, m_z
                lows[y], lows_z[y] = low, low_z
                boths[y], boths_z[y] = m + low, m_z + low_z
        for q in range(rowcount):
            reacts = paired(tiles[blocks + q], tiles[blocks + rowcount + q])
            for k, react in enumerate(reacts):
                y = CY * q + k
                around = (boths[y] + boths_z[y]) + (boths[(y - 1) % planes] + boths_z[(y - 1) % planes])
                diag[y] = react - 4.0 * around

        inbox[me] = outbox[rank]
        for o in range(1, blocks):
            b = lax.rem(me + o, blocks)
            pltpu.make_async_remote_copy(
                src_ref=outbox.at[0], dst_ref=inbox.at[b],
                send_sem=out_send.at[0], recv_sem=out_recv.at[b],
                device_id=block(b), device_id_type=MESH,
            ).wait_recv()
        for q in range(rowcount):
            for k, value in enumerate(paired(inbox[q], inbox[rowcount + q])):
                bases[0, CY * q + k] = value

        def apply_operator(source, sink):
            taken = {}

            def around(y):
                y = y % planes
                if y not in taken:
                    v = source(y)
                    above, below = turned(v, -SUB), turned(v, SUB)
                    taken[y] = (v, above, below, v + above, v + below)
                return taken[y]

            for y in range(planes):
                v, above, below, _, _ = around(y)
                _, next_above, next_below, next_up, next_down = around(y + 1)
                _, last_above, last_below, last_up, last_down = around(y - 1)
                sides = [above + next_up, below + next_down, above + last_up, below + last_down]
                diagonal = [next_above, next_below, last_above, last_below]

                def weighed(a, b, values, y=y):
                    z = (y - 1) % planes
                    products = [
                        c * value for c, value in zip((a[y], b[y], a[z], b[z]), values)
                    ]
                    return (products[0] + products[1]) + (products[2] + products[3])

                ahead = turned(weighed(lows, lows_z, sides), -1, 0)
                behind = turned(weighed(masses, masses_z, sides), 1, 0)
                middle = weighed(boths, boths_z, diagonal) + diag[y] * v
                sink(y, middle + (ahead + behind))

        scale, steps = chebyshev_steps()
        square, cross = Total(), Total()

        def first_image(y, image):
            residuals[y] = image
            square.add(image * image)
            cross.add(bases[0, y] * image)

        apply_operator(lambda y: bases[0, y], first_image)
        square, cross = summed(square, cross)
        inverse = cross / square
        opening = scale * inverse

        omegas, squares = [], []
        for sweep in range(SWEEPS):
            along, length, begin = Total(), Total(), Total()
            for step in range(DEGREE):
                here, there = directions.at[step % 2], directions.at[(step + 1) % 2]

                def finish(y, image, step=step, here=here, there=there, sweep=sweep):
                    residual = (bases[sweep, y] if step == 0 else residuals[y]) - image
                    if step + 1 < DEGREE:
                        direction = here[y]
                        keep, gain = steps[step]
                        following = keep * direction + (gain * inverse) * residual
                        residuals[y] = residual
                        there[y] = following
                        so_far = direction if step == 0 else corrections[sweep, y]
                        corrections[sweep, y] = so_far + following
                    else:
                        start = bases[sweep, y]
                        change = start - residual
                        changes[y] = change
                        along.add(start * change)
                        length.add(change * change)

                if sweep == 0 and step == 0:
                    for y in range(planes):
                        here[y] = opening * bases[0, y]
                        finish(y, opening * residuals[y])
                else:
                    apply_operator(lambda y, here=here: here[y], finish)
            along, length = summed(along, length)
            omega = along / length
            omegas.append(omega)
            if sweep + 1 < SWEEPS:
                for y in range(planes):
                    base = bases[sweep, y] - omega * changes[y]
                    bases[sweep + 1, y] = base
                    directions[0, y] = opening * base
                    begin.add(base * base)
                began = over_z(begin.folded())
        group = tile_iota(1) // SUB
        last = jnp.maximum(began - omega * along, 0.0)
        rms = jnp.where(group == rank, began, jnp.where(group == rank + leaders, last, 0.0))
        rms = jnp.sqrt(rms / total)[0:1]
        for q in range(rowcount):
            values = [
                omegas[0] * corrections[0, CY * q + k] + omegas[1] * corrections[1, CY * q + k]
                for k in range(CY)
            ]
            for p, tile in enumerate(paired(*values)):
                solved[p * rowcount + q, 0:SUB] = tile
                solved[p * rowcount + q, SUB : SUB + 1] = rms
        for o in range(1, leaders):
            reply(place_of(lax.rem(rank + o, leaders))).start()
        for g in range(groups):
            for r in range(heads, rowcount):
                reply(g * rowcount + r).start()
        answers[rank] = solved[me]

    def await_reply(t):
        pltpu.make_async_remote_copy(
            src_ref=solved.at[0], dst_ref=answers.at[t],
            send_sem=back_send.at[0], recv_sem=back_recv.at[t],
            device_id=leader(t), device_id_type=MESH,
        ).wait_recv()

    for o in range(1, leaders):
        await_reply(lax.rem(rank + o, leaders))

    @pl.when(jnp.logical_not(leading))
    def _():
        await_reply(lax.rem(rank, leaders))

    whole = jnp.concatenate([exchanged(answers[t, 0:SUB]) for t in range(leaders)], axis=0)
    whole = jnp.concatenate(thirds(whole), axis=0)
    whole = lax.dot_general(
        whole, order[...], (((1,), (1,)), ((), ())), preferred_element_type=jnp.float32
    )
    packed_ref[0:nrhs] = added([whole[k * nrhs : (k + 1) * nrhs] for k in range(3)])
    line = answers[0, SUB : SUB + 1]
    for t in range(1, leaders):
        line = line + answers[t, SUB : SUB + 1]
    packed_ref[nrhs : nrhs + SUB] = jnp.concatenate(
        [line, turned(line, count // 2), jnp.zeros((SUB - 2, count), jnp.float32)], axis=0
    )

    for send in (post_aux, post_field):
        for o in range(1, leaders):
            send(o).wait_send()

        @pl.when(jnp.logical_not(leading))
        def _(send=send):
            send(0).wait_send()

    @pl.when(leading)
    def _():
        for o in range(1, blocks):
            reply(lax.rem(me + o, blocks)).wait_send()


def unpack(packed_ref, out_ref, rms_ref):
    nrhs = out_ref.shape[0]
    out_ref[...] = packed_ref[:nrhs]
    rms_ref[...] = packed_ref[nrhs : nrhs + SWEEPS, :nrhs]


def whole_sweeps(groups, rowcount, right_side, links, coefs, reaction):
    nrhs, count = right_side.shape
    leaders = nrhs // SUB
    blocks = groups * rowcount
    planes = rowcount * CY
    dma = pltpu.SemaphoreType.DMA
    vmem = pl.BlockSpec(memory_space=pltpu.VMEM)

    def space(*shape):
        return pltpu.VMEM(shape, jnp.float32)

    plane = space(planes, SUB, count)
    twice = space(SWEEPS, planes, SUB, count)
    packed = pl.pallas_call(
        functools.partial(kernel, groups, rowcount, count * groups * rowcount),
        out_shape=jax.ShapeDtypeStruct((nrhs + SUB, count), jnp.float32),
        in_specs=[pl.BlockSpec(memory_space=pl.ANY)] * 4,
        out_specs=vmem,
        scratch_shapes=[
            space(nrhs, count), pltpu.VMEM(links.shape, jnp.int32), space(1, count), space(1, count),
            space(2, count), space(blocks, 2, count),
            space(leaders, SUB, count), space(blocks, SUB, count),
            space(leaders, SUB + 1, count), space(blocks, SUB + 1, count),
            space(count, count), space(2 * count, count), space(2, 2 * blocks, count),
            plane, plane, plane, plane, plane, plane, plane,
            twice, plane, space(2, planes, SUB, count), twice, plane,
            dma((4,)), dma((leaders,)), dma((blocks,)), dma((leaders,)), dma((blocks,)),
            dma((blocks,)), dma((leaders,)),
        ],
        compiler_params=pltpu.CompilerParams(collective_id=0, has_side_effects=True),
    )(right_side, links, coefs.reshape(1, count), reaction.reshape(1, count))
    return pl.pallas_call(
        unpack,
        out_shape=(
            jax.ShapeDtypeStruct((nrhs, count), jnp.float32),
            jax.ShapeDtypeStruct((SWEEPS, nrhs), jnp.float32),
        ),
        in_specs=[vmem],
        out_specs=(vmem, vmem),
    )(packed)


def in_one_kernel(mesh):
    return mesh.shape["grp"] == SUB // CX and 2 * SUB <= mesh.shape["row"] <= 4 * SUB


def solution(mesh):
    body = on_device
    if in_one_kernel(mesh):
        body = functools.partial(whole_sweeps, mesh.shape["grp"], mesh.shape["row"])
    return jax.shard_map(
        body,
        mesh=mesh,
        in_specs=(
            P(None, ("grp", "row")),
            P(None, ("grp", "row")),
            P(("grp", "row")),
            P(("grp", "row")),
        ),
        out_specs=(P(None, ("grp", "row")), P()),
        check_vma=False,
    )
```

```python
import functools
import math

import jax
import jax.numpy as jnp
import numpy as np
from jax import lax
from jax.experimental import pallas as pl
from jax.experimental.pallas import tpu as pltpu
from jax.sharding import PartitionSpec as P

SWEEPS = 2
DEGREE = 4
CX, CY, CZ = 4, 2, 16
SUB, LANES = 8, 128
MESH = pl.DeviceIdType.MESH
HIGHEST = lax.Precision.HIGHEST


def shifted(block, axis, distance):
    devices = range(lax.axis_size(axis))
    route = [((i - distance) % len(devices), i) for i in devices]
    return lax.ppermute(block, axis, route)


def element_matrix():
    node_ids = np.arange(8)
    corner = np.stack([node_ids % 2, node_ids // 2 % 2, node_ids // 4], axis=1)
    gauss_points = np.array([0.5 - 0.5 / math.sqrt(3.0), 0.5 + 0.5 / math.sqrt(3.0)])
    stiffness = np.zeros((8, 8))
    for q in range(8):
        quad_point = gauss_points[np.array([q % 2, q // 2 % 2, q // 4])]
        values = np.where(corner > 0.5, quad_point, 1.0 - quad_point)
        slopes = np.where(corner > 0.5, 1.0, -1.0)
        gradient = np.stack(
            [
                slopes[:, 0] * values[:, 1] * values[:, 2],
                values[:, 0] * slopes[:, 1] * values[:, 2],
                values[:, 0] * values[:, 1] * slopes[:, 2],
            ],
            axis=1,
        )
        stiffness = stiffness + gradient @ gradient.T / 8.0
    return stiffness


def element_images(window, offsets, weights, stiffness):
    corners = window[:, offsets]
    images = (
        jnp.einsum("ml,rle->rme", stiffness, corners, precision=lax.Precision.HIGHEST) * weights
    )
    return jnp.zeros_like(window).at[:, offsets].add(images)


def on_device(right_side, links, coefs, reaction):
    stiffness = jnp.asarray(element_matrix(), dtype=jnp.float32)
    count = right_side.shape[1]
    groups = lax.axis_size("grp")
    rowcount = lax.axis_size("row")
    group_id = lax.axis_index("grp")
    row_id = lax.axis_index("row")
    total = count * groups * rowcount
    owner = links // count
    slot = links % count
    first = jnp.mod(owner // rowcount - group_id, groups)
    second = jnp.mod(owner % rowcount - row_id, rowcount)
    offsets = (first * 2 + second) * count + slot

    def apply_operator(field):
        above_row = shifted(field, "row", -1)
        upper = shifted(jnp.stack([field, above_row], axis=0), "grp", -1)
        window = jnp.concatenate([field, above_row, upper[0], upper[1]], axis=1)
        summed = element_images(window, offsets, coefs, stiffness)
        back = shifted(
            jnp.stack([summed[:, 2 * count : 3 * count], summed[:, 3 * count :]], axis=0), "grp", 1
        )
        first_col = summed[:, :count] + back[0]
        second_col = summed[:, count : 2 * count] + back[1]
        first_col = first_col + shifted(second_col, "row", 1)
        return first_col + reaction * field

    image = apply_operator(right_side)
    cross, square = lax.psum(
        (jnp.sum(right_side * image, axis=1), jnp.sum(image * image, axis=1)), ("grp", "row")
    )
    theta = square / cross
    upper = (1.5 * theta)[:, None]
    lower = upper / 10.0
    center = (upper + lower) / 2.0
    half = (upper - lower) / 2.0
    sigma = center / half
    solution = jnp.zeros_like(right_side)
    residual = right_side
    history = []
    for sweep in range(SWEEPS):
        start = residual
        correction = jnp.zeros_like(right_side)
        rho_now = 1.0 / sigma
        direction = residual / center
        for step in range(DEGREE):
            correction = correction + direction
            residual = residual - apply_operator(direction)
            if step + 1 < DEGREE:
                rho_next = 1.0 / (2.0 * sigma - rho_now)
                direction = rho_next * rho_now * direction + 2.0 * rho_next / half * residual
                rho_now = rho_next
        change = start - residual
        along, length, begin = lax.psum(
            (
                jnp.sum(start * change, axis=1),
                jnp.sum(change * change, axis=1),
                jnp.sum(start * start, axis=1),
            ),
            ("grp", "row"),
        )
        omega = along / length
        residual = start - omega[:, None] * change
        squares = begin - 2.0 * omega * along + omega * omega * length
        solution = solution + omega[:, None] * correction
        history.append(jnp.sqrt(squares / total))
    return (solution, jnp.stack(history, axis=0))


def thirds(a):
    high = a.astype(jnp.bfloat16).astype(jnp.float32)
    rest = a - high
    middle = rest.astype(jnp.bfloat16).astype(jnp.float32)
    return [high, middle, rest - middle]


def added(parts):
    high, middle, low = parts
    return high + middle + low


def turned(a, distance, axis=1):
    return pltpu.roll(a, distance % a.shape[axis], axis)


def tile_iota(axis):
    return lax.broadcasted_iota(jnp.int32, (SUB, LANES), axis)


def exchanged(tile):
    sub, low = tile_iota(0), tile_iota(1)
    for unit, radix in ((1, 4), (4, 2)):
        ahead = low // unit % radix - sub // unit % radix
        result = tile
        for k in range(1 - radix, radix):
            if k:
                moved = turned(turned(tile, -k * unit, 0), k * unit)
                result = jnp.where(ahead == k, moved, result)
        tile = result
    return tile


def paired(first, second):
    top = tile_iota(0) < SUB // 2
    return (
        jnp.where(top, first, turned(second, SUB // 2, 0)),
        jnp.where(top, turned(first, SUB // 2, 0), second),
    )


def chebyshev_steps():
    sigma = (1.5 + 0.15) / (1.5 - 0.15)
    rho_now = 1.0 / sigma
    steps = []
    for _ in range(DEGREE - 1):
        rho_next = 1.0 / (2.0 * sigma - rho_now)
        steps.append((rho_next * rho_now, 2.0 * rho_next / ((1.5 - 0.15) / 2.0)))
        rho_now = rho_next
    return 2.0 / (1.5 + 0.15), steps


class Total:
    def __init__(self):
        self.parts = [None] * 4
        self.at = 0

    def add(self, value):
        k = self.at % 4
        self.parts[k] = value if self.parts[k] is None else self.parts[k] + value
        self.at += 1

    def folded(self):
        a, b, c, d = self.parts
        value = (a + b) + (c + d)
        for bit in (4, 2, 1):
            value = value + turned(value, bit, 0)
        return value


def over_z(value):
    parts = [value] + [turned(value, SUB * k) for k in range(1, LANES // SUB)]
    while len(parts) > 1:
        parts = [a + b for a, b in zip(parts[::2], parts[1::2])]
    return parts[0]


def summed(first, second):
    top = tile_iota(0) < SUB // 2
    both = over_z(jnp.where(top, first.folded(), second.folded()))
    other = turned(both, SUB // 2, 0)
    return jnp.where(top, both, other), jnp.where(top, other, both)


def kernel(
    groups, rowcount, total,
    right_hbm, links_hbm, coefs_hbm, react_hbm,
    solution_ref, rms_ref,
    right_ref, links_ref, coefs_ref, react_ref,
    auxout, auxin, outbox, inbox, answers, solved, order, spread, wide,
    masses, masses_z, lows, lows_z, boths, boths_z, diag,
    bases, changes, directions, corrections, residuals,
    in_sem, aux_send, aux_recv, out_send, out_recv, back_send, back_recv,
):
    nrhs, count = right_ref.shape
    leaders = nrhs // SUB
    heads = leaders // groups
    blocks = groups * rowcount
    planes = rowcount * CY
    grp = lax.axis_index("grp")
    row = lax.axis_index("row")
    me = grp * rowcount + row
    leading = row < heads
    rank = grp * heads + row

    def leader(t):
        return (t // heads, lax.rem(t, heads))

    def block(b):
        return (b // rowcount, lax.rem(b, rowcount))

    def place_of(t):
        return (t // heads) * rowcount + lax.rem(t, heads)

    barrier = pltpu.get_barrier_semaphore()

    @pl.when(leading)
    def _():
        def nearness(place):
            d, o = place
            return abs(2 * o - rowcount) - 2 * heads * d - heads * (o % heads == heads // 2)

        peers = [(d, o) for d in range(groups) for o in range(rowcount) if d or o]
        for d, o in sorted(peers, key=nearness):
            peer = (lax.rem(grp + d, groups), lax.rem(row + o, rowcount))
            pl.semaphore_signal(barrier, inc=1, device_id=peer, device_id_type=MESH)

    loads = [
        pltpu.make_async_copy(source, target, in_sem.at[k])
        for k, (source, target) in enumerate(
            [(links_hbm, links_ref), (coefs_hbm, coefs_ref), (react_hbm, react_ref), (right_hbm, right_ref)]
        )
    ]
    for load in loads:
        load.start()

    lane = lax.broadcasted_iota(jnp.int32, (count, count), 1)
    down = lax.broadcasted_iota(jnp.int32, (count, count), 0)
    same_z = (down // SUB == lane // SUB).astype(jnp.float32)
    spread[0:count] = same_z
    spread[count : 2 * count] = same_z
    low = tile_iota(1)
    element = ((low % CX) * CY + low // CX % CY) * CZ + low // SUB

    def to_lanes(line):
        return jnp.take_along_axis(jnp.broadcast_to(line, (SUB, count)), element, axis=1)[0:1]

    for load in loads[:3]:
        load.wait()
    slots = to_lanes(links_ref[0:1, :] - me * count)
    order[...] = (down == slots).astype(jnp.float32)
    mass = to_lanes(coefs_ref[...] * (-1.0 / 12.0))
    react = thirds(react_ref[...])
    react = jnp.concatenate(react + [jnp.zeros((SUB - 3, count), jnp.float32)], axis=0)
    loads[3].wait()
    stack = jnp.concatenate([react] + thirds(right_ref[...]), axis=0)
    stack = jnp.dot(stack, order[...], preferred_element_type=jnp.float32)
    react = added([stack[k : k + 1] for k in range(3)])
    auxout[...] = jnp.concatenate([mass, react], axis=0)
    field = added([stack[SUB + k * nrhs : SUB + (k + 1) * nrhs] for k in range(3)])

    def post(o, source, target, send, recv):
        t = lax.rem(rank + o, leaders)
        return pltpu.make_async_remote_copy(
            src_ref=source(t), dst_ref=target.at[me], send_sem=send.at[t], recv_sem=recv,
            device_id=leader(t), device_id_type=MESH,
        )

    def post_aux(o):
        return post(o, lambda t: auxout, auxin, aux_send, aux_recv.at[me])

    def post_field(o):
        return post(o, lambda t: outbox.at[t], inbox, out_send, out_recv.at[me])

    for t in range(leaders):
        outbox[t] = exchanged(field[t * SUB : (t + 1) * SUB])
    pl.semaphore_wait(barrier, jnp.where(leading, leaders - 1, leaders))

    for send in (post_aux, post_field):
        for o in range(1, leaders):
            send(o).start()

        @pl.when(jnp.logical_not(leading))
        def _(send=send):
            send(0).start()

    def reply(b):
        return pltpu.make_async_remote_copy(
            src_ref=solved.at[b], dst_ref=answers.at[rank],
            send_sem=back_send.at[b], recv_sem=back_recv.at[rank],
            device_id=block(b), device_id_type=MESH,
        )

    @pl.when(leading)
    def _():
        auxin[me] = auxout[...]
        for o in range(1, blocks):
            b = lax.rem(me + o, blocks)
            pltpu.make_async_remote_copy(
                src_ref=auxout, dst_ref=auxin.at[b],
                send_sem=aux_send.at[0], recv_sem=aux_recv.at[b],
                device_id=block(b), device_id_type=MESH,
            ).wait_recv()

        own = tile_iota(1) % SUB == tile_iota(0)
        for k in range(2):
            high, middle, _ = thirds(auxin[:, k, :])
            wide[0, k * blocks : (k + 1) * blocks] = high
            wide[1, k * blocks : (k + 1) * blocks] = middle
        pieces = [
            jnp.concatenate(
                [jnp.where(own, wide[part, k : k + 1, :], 0.0) for k in range(2 * blocks)], axis=0
            )
            for part in range(2)
        ]
        tiles = jnp.dot(
            jnp.concatenate(pieces, axis=1), spread[...], preferred_element_type=jnp.float32
        )
        tiles = [tiles[k * SUB : (k + 1) * SUB] for k in range(2 * blocks)]
        for q in range(rowcount):
            for k, m in enumerate(paired(tiles[q], tiles[rowcount + q])):
                y = CY * q + k
                m_z = turned(m, SUB)
                low, low_z = turned(m, 1, 0), turned(m_z, 1, 0)
                masses[y], masses_z[y] = m, m_z
                lows[y], lows_z[y] = low, low_z
                boths[y], boths_z[y] = m + low, m_z + low_z
        for q in range(rowcount):
            reacts = paired(tiles[blocks + q], tiles[blocks + rowcount + q])
            for k, react in enumerate(reacts):
                y = CY * q + k
                around = (boths[y] + boths_z[y]) + (boths[(y - 1) % planes] + boths_z[(y - 1) % planes])
                diag[y] = react - 4.0 * around

        inbox[me] = outbox[rank]
        for o in range(1, blocks):
            b = lax.rem(me + o, blocks)
            pltpu.make_async_remote_copy(
                src_ref=outbox.at[0], dst_ref=inbox.at[b],
                send_sem=out_send.at[0], recv_sem=out_recv.at[b],
                device_id=block(b), device_id_type=MESH,
            ).wait_recv()
        for q in range(rowcount):
            for k, value in enumerate(paired(inbox[q], inbox[rowcount + q])):
                bases[0, CY * q + k] = value

        def apply_operator(source, sink):
            taken = {}

            def around(y):
                y = y % planes
                if y not in taken:
                    v = source(y)
                    above, below = turned(v, -SUB), turned(v, SUB)
                    taken[y] = (v, above, below, v + above, v + below)
                return taken[y]

            for y in range(planes):
                v, above, below, _, _ = around(y)
                _, next_above, next_below, next_up, next_down = around(y + 1)
                _, last_above, last_below, last_up, last_down = around(y - 1)
                sides = [above + next_up, below + next_down, above + last_up, below + last_down]
                diagonal = [next_above, next_below, last_above, last_below]

                def weighed(a, b, values, y=y):
                    z = (y - 1) % planes
                    products = [
                        c * value for c, value in zip((a[y], b[y], a[z], b[z]), values)
                    ]
                    return (products[0] + products[1]) + (products[2] + products[3])

                ahead = turned(weighed(lows, lows_z, sides), -1, 0)
                behind = turned(weighed(masses, masses_z, sides), 1, 0)
                middle = weighed(boths, boths_z, diagonal) + diag[y] * v
                sink(y, middle + (ahead + behind))

        scale, steps = chebyshev_steps()
        square, cross = Total(), Total()

        def first_image(y, image):
            residuals[y] = image
            square.add(image * image)
            cross.add(bases[0, y] * image)

        apply_operator(lambda y: bases[0, y], first_image)
        square, cross = summed(square, cross)
        inverse = cross / square
        opening = scale * inverse

        omegas, squares = [], []
        for sweep in range(SWEEPS):
            along, length, begin = Total(), Total(), Total()
            for step in range(DEGREE):
                here, there = directions.at[step % 2], directions.at[(step + 1) % 2]

                def finish(y, image, step=step, here=here, there=there, sweep=sweep):
                    residual = (bases[sweep, y] if step == 0 else residuals[y]) - image
                    if step + 1 < DEGREE:
                        direction = here[y]
                        keep, gain = steps[step]
                        following = keep * direction + (gain * inverse) * residual
                        residuals[y] = residual
                        there[y] = following
                        so_far = direction if step == 0 else corrections[sweep, y]
                        corrections[sweep, y] = so_far + following
                    else:
                        start = bases[sweep, y]
                        change = start - residual
                        changes[y] = change
                        along.add(start * change)
                        length.add(change * change)

                if sweep == 0 and step == 0:
                    for y in range(planes):
                        here[y] = opening * bases[0, y]
                        finish(y, opening * residuals[y])
                else:
                    apply_operator(lambda y, here=here: here[y], finish)
            along, length = summed(along, length)
            omega = along / length
            omegas.append(omega)
            if sweep + 1 < SWEEPS:
                for y in range(planes):
                    base = bases[sweep, y] - omega * changes[y]
                    bases[sweep + 1, y] = base
                    directions[0, y] = opening * base
                    begin.add(base * base)
                began = over_z(begin.folded())
        group = tile_iota(1) // SUB
        last = jnp.maximum(began - omega * along, 0.0)
        rms = jnp.where(group == rank, began, jnp.where(group == rank + leaders, last, 0.0))
        rms = jnp.sqrt(rms / total)[0:1]
        for q in range(rowcount):
            values = [
                omegas[0] * corrections[0, CY * q + k] + omegas[1] * corrections[1, CY * q + k]
                for k in range(CY)
            ]
            for p, tile in enumerate(paired(*values)):
                solved[p * rowcount + q, 0:SUB] = tile
                solved[p * rowcount + q, SUB : SUB + 1] = rms
        for o in range(1, leaders):
            reply(place_of(lax.rem(rank + o, leaders))).start()
        for g in range(groups):
            for r in range(heads, rowcount):
                reply(g * rowcount + r).start()
        answers[rank] = solved[me]

    def await_reply(t):
        pltpu.make_async_remote_copy(
            src_ref=solved.at[0], dst_ref=answers.at[t],
            send_sem=back_send.at[0], recv_sem=back_recv.at[t],
            device_id=leader(t), device_id_type=MESH,
        ).wait_recv()

    for o in range(1, leaders):
        await_reply(lax.rem(rank + o, leaders))

    @pl.when(jnp.logical_not(leading))
    def _():
        await_reply(lax.rem(rank, leaders))

    whole = jnp.concatenate([exchanged(answers[t, 0:SUB]) for t in range(leaders)], axis=0)
    whole = jnp.concatenate(thirds(whole), axis=0)
    whole = lax.dot_general(
        whole, order[...], (((1,), (1,)), ((), ())), preferred_element_type=jnp.float32
    )
    solution_ref[...] = added([whole[k * nrhs : (k + 1) * nrhs] for k in range(3)])
    line = answers[0, SUB : SUB + 1]
    for t in range(1, leaders):
        line = line + answers[t, SUB : SUB + 1]
    other = turned(line, count // 2)
    rms_ref[...] = jnp.concatenate([line, other], axis=0)[:, :nrhs]

    for send in (post_aux, post_field):
        for o in range(1, leaders):
            send(o).wait_send()

        @pl.when(jnp.logical_not(leading))
        def _(send=send):
            send(0).wait_send()

    @pl.when(leading)
    def _():
        for o in range(1, blocks):
            reply(lax.rem(me + o, blocks)).wait_send()


def write_out(solution_ref, rms_ref, out_hbm, rms_hbm, sems):
    copies = [
        pltpu.make_async_copy(solution_ref, out_hbm, sems.at[0]),
        pltpu.make_async_copy(rms_ref, rms_hbm, sems.at[1]),
    ]
    for copy in copies:
        copy.start()
    for copy in copies:
        copy.wait()


def whole_sweeps(groups, rowcount, right_side, links, coefs, reaction):
    nrhs, count = right_side.shape
    leaders = nrhs // SUB
    blocks = groups * rowcount
    planes = rowcount * CY
    dma = pltpu.SemaphoreType.DMA
    vmem = pl.BlockSpec(memory_space=pltpu.VMEM)

    def space(*shape):
        return pltpu.VMEM(shape, jnp.float32)

    plane = space(planes, SUB, count)
    twice = space(SWEEPS, planes, SUB, count)
    found = pl.pallas_call(
        functools.partial(kernel, groups, rowcount, count * groups * rowcount),
        out_shape=(pltpu.VMEM((nrhs, count), jnp.float32), pltpu.VMEM((SWEEPS, nrhs), jnp.float32)),
        in_specs=[pl.BlockSpec(memory_space=pl.ANY)] * 4,
        out_specs=(vmem, vmem),
        scratch_shapes=[
            space(nrhs, count), pltpu.VMEM(links.shape, jnp.int32), space(1, count), space(1, count),
            space(2, count), space(blocks, 2, count),
            space(leaders, SUB, count), space(blocks, SUB, count),
            space(leaders, SUB + 1, count), space(blocks, SUB + 1, count),
            space(count, count), space(2 * count, count), space(2, 2 * blocks, count),
            plane, plane, plane, plane, plane, plane, plane,
            twice, plane, space(2, planes, SUB, count), twice, plane,
            dma((4,)), dma((leaders,)), dma((blocks,)), dma((leaders,)), dma((blocks,)),
            dma((blocks,)), dma((leaders,)),
        ],
        compiler_params=pltpu.CompilerParams(collective_id=0, has_side_effects=True),
    )(right_side, links, coefs.reshape(1, count), reaction.reshape(1, count))
    return pl.pallas_call(
        write_out,
        out_shape=(
            jax.ShapeDtypeStruct((nrhs, count), jnp.float32),
            jax.ShapeDtypeStruct((SWEEPS, nrhs), jnp.float32),
        ),
        in_specs=[vmem, vmem],
        out_specs=[pl.BlockSpec(memory_space=pl.ANY)] * 2,
        scratch_shapes=[dma((2,))],
    )(*[pltpu.with_memory_space_constraint(f, pltpu.VMEM) for f in found])


def in_one_kernel(mesh):
    return mesh.shape["grp"] == SUB // CX and 2 * SUB <= mesh.shape["row"] <= 4 * SUB


def solution(mesh):
    body = on_device
    if in_one_kernel(mesh):
        body = functools.partial(whole_sweeps, mesh.shape["grp"], mesh.shape["row"])
    return jax.shard_map(
        body,
        mesh=mesh,
        in_specs=(
            P(None, ("grp", "row")),
            P(None, ("grp", "row")),
            P(("grp", "row")),
            P(("grp", "row")),
        ),
        out_specs=(P(None, ("grp", "row")), P()),
        check_vma=False,
    )
```

```python
import functools
import math

import jax
import jax.numpy as jnp
import numpy as np
from jax import lax
from jax.experimental import pallas as pl
from jax.experimental.pallas import tpu as pltpu
from jax.sharding import PartitionSpec as P

SWEEPS = 2
DEGREE = 4
CX, CY, CZ = 4, 2, 16
SUB, LANES = 8, 128
MESH = pl.DeviceIdType.MESH
HIGHEST = lax.Precision.HIGHEST


def shifted(block, axis, distance):
    devices = range(lax.axis_size(axis))
    route = [((i - distance) % len(devices), i) for i in devices]
    return lax.ppermute(block, axis, route)


def element_matrix():
    node_ids = np.arange(8)
    corner = np.stack([node_ids % 2, node_ids // 2 % 2, node_ids // 4], axis=1)
    gauss_points = np.array([0.5 - 0.5 / math.sqrt(3.0), 0.5 + 0.5 / math.sqrt(3.0)])
    stiffness = np.zeros((8, 8))
    for q in range(8):
        quad_point = gauss_points[np.array([q % 2, q // 2 % 2, q // 4])]
        values = np.where(corner > 0.5, quad_point, 1.0 - quad_point)
        slopes = np.where(corner > 0.5, 1.0, -1.0)
        gradient = np.stack(
            [
                slopes[:, 0] * values[:, 1] * values[:, 2],
                values[:, 0] * slopes[:, 1] * values[:, 2],
                values[:, 0] * values[:, 1] * slopes[:, 2],
            ],
            axis=1,
        )
        stiffness = stiffness + gradient @ gradient.T / 8.0
    return stiffness


def element_images(window, offsets, weights, stiffness):
    corners = window[:, offsets]
    images = (
        jnp.einsum("ml,rle->rme", stiffness, corners, precision=lax.Precision.HIGHEST) * weights
    )
    return jnp.zeros_like(window).at[:, offsets].add(images)


def on_device(right_side, links, coefs, reaction):
    stiffness = jnp.asarray(element_matrix(), dtype=jnp.float32)
    count = right_side.shape[1]
    groups = lax.axis_size("grp")
    rowcount = lax.axis_size("row")
    group_id = lax.axis_index("grp")
    row_id = lax.axis_index("row")
    total = count * groups * rowcount
    owner = links // count
    slot = links % count
    first = jnp.mod(owner // rowcount - group_id, groups)
    second = jnp.mod(owner % rowcount - row_id, rowcount)
    offsets = (first * 2 + second) * count + slot

    def apply_operator(field):
        above_row = shifted(field, "row", -1)
        upper = shifted(jnp.stack([field, above_row], axis=0), "grp", -1)
        window = jnp.concatenate([field, above_row, upper[0], upper[1]], axis=1)
        summed = element_images(window, offsets, coefs, stiffness)
        back = shifted(
            jnp.stack([summed[:, 2 * count : 3 * count], summed[:, 3 * count :]], axis=0), "grp", 1
        )
        first_col = summed[:, :count] + back[0]
        second_col = summed[:, count : 2 * count] + back[1]
        first_col = first_col + shifted(second_col, "row", 1)
        return first_col + reaction * field

    image = apply_operator(right_side)
    cross, square = lax.psum(
        (jnp.sum(right_side * image, axis=1), jnp.sum(image * image, axis=1)), ("grp", "row")
    )
    theta = square / cross
    upper = (1.5 * theta)[:, None]
    lower = upper / 10.0
    center = (upper + lower) / 2.0
    half = (upper - lower) / 2.0
    sigma = center / half
    solution = jnp.zeros_like(right_side)
    residual = right_side
    history = []
    for sweep in range(SWEEPS):
        start = residual
        correction = jnp.zeros_like(right_side)
        rho_now = 1.0 / sigma
        direction = residual / center
        for step in range(DEGREE):
            correction = correction + direction
            residual = residual - apply_operator(direction)
            if step + 1 < DEGREE:
                rho_next = 1.0 / (2.0 * sigma - rho_now)
                direction = rho_next * rho_now * direction + 2.0 * rho_next / half * residual
                rho_now = rho_next
        change = start - residual
        along, length, begin = lax.psum(
            (
                jnp.sum(start * change, axis=1),
                jnp.sum(change * change, axis=1),
                jnp.sum(start * start, axis=1),
            ),
            ("grp", "row"),
        )
        omega = along / length
        residual = start - omega[:, None] * change
        squares = begin - 2.0 * omega * along + omega * omega * length
        solution = solution + omega[:, None] * correction
        history.append(jnp.sqrt(squares / total))
    return (solution, jnp.stack(history, axis=0))


def thirds(a):
    high = a.astype(jnp.bfloat16).astype(jnp.float32)
    rest = a - high
    middle = rest.astype(jnp.bfloat16).astype(jnp.float32)
    return [high, middle, rest - middle]


def added(parts):
    high, middle, low = parts
    return high + middle + low


def turned(a, distance, axis=1):
    return pltpu.roll(a, distance % a.shape[axis], axis)


def tile_iota(axis):
    return lax.broadcasted_iota(jnp.int32, (SUB, LANES), axis)


def exchanged(tile):
    sub, low = tile_iota(0), tile_iota(1)
    for unit, radix in ((1, 4), (4, 2)):
        ahead = low // unit % radix - sub // unit % radix
        result = tile
        for k in range(1 - radix, radix):
            if k:
                moved = turned(turned(tile, -k * unit, 0), k * unit)
                result = jnp.where(ahead == k, moved, result)
        tile = result
    return tile


def paired(first, second):
    top = tile_iota(0) < SUB // 2
    return (
        jnp.where(top, first, turned(second, SUB // 2, 0)),
        jnp.where(top, turned(first, SUB // 2, 0), second),
    )


def chebyshev_weights():
    center, half = (1.5 + 0.15) / 2.0, (1.5 - 0.15) / 2.0
    sigma = center / half
    rho_now = 1.0 / sigma
    direction, residual = np.zeros(DEGREE + 1), np.zeros(DEGREE + 1)
    correction = np.zeros(DEGREE + 1)
    residual[0], direction[0] = 1.0, 1.0 / center
    for _ in range(DEGREE):
        correction = correction + direction
        residual = residual - np.roll(direction, 1)
        rho_next = 1.0 / (2.0 * sigma - rho_now)
        direction = rho_next * rho_now * direction + 2.0 * rho_next / half * residual
        rho_now = rho_next
    return [float(b) for b in correction[:DEGREE]], [-float(c) for c in residual[1:]]


class Total:
    def __init__(self):
        self.parts = [None] * 4
        self.at = 0

    def add(self, value):
        k = self.at % 4
        self.parts[k] = value if self.parts[k] is None else self.parts[k] + value
        self.at += 1

    def folded(self):
        a, b, c, d = self.parts
        value = (a + b) + (c + d)
        for bit in (4, 2, 1):
            value = value + turned(value, bit, 0)
        return value


def over_z(value):
    parts = [value] + [turned(value, SUB * k) for k in range(1, LANES // SUB)]
    while len(parts) > 1:
        parts = [a + b for a, b in zip(parts[::2], parts[1::2])]
    return parts[0]


def summed(first, second):
    top = tile_iota(0) < SUB // 2
    both = over_z(jnp.where(top, first.folded(), second.folded()))
    other = turned(both, SUB // 2, 0)
    return jnp.where(top, both, other), jnp.where(top, other, both)


def kernel(
    groups, rowcount, total,
    right_hbm, links_hbm, coefs_hbm, react_hbm,
    solution_ref, rms_ref,
    right_ref, links_ref, coefs_ref, react_ref,
    auxout, auxin, outbox, inbox, answers, solved, order, spread, wide,
    masses, masses_z, lows, lows_z, boths, boths_z, diag,
    bases, changes, corrections, powers, mixes,
    in_sem, aux_send, aux_recv, out_send, out_recv, back_send, back_recv,
):
    nrhs, count = right_ref.shape
    leaders = nrhs // SUB
    near, second = leaders - CY, CY
    blocks = groups * rowcount
    planes = rowcount * CY
    grp = lax.axis_index("grp")
    row = lax.axis_index("row")
    me = grp * rowcount + row
    leading = row < jnp.where(grp == 0, near, second)
    rank = jnp.where(grp == 0, row, near + row)

    def leader(t):
        if isinstance(t, int):
            return (0, t) if t < near else (1, t - near)
        return (jnp.where(t < near, 0, 1), jnp.where(t < near, t, t - near))

    def block(b):
        return (b // rowcount, lax.rem(b, rowcount))

    def place_of(t):
        return jnp.where(t < near, t, rowcount + t - near)

    def another(k):
        return jnp.where(k < rank, k, k + 1)

    barrier = pltpu.get_barrier_semaphore()

    @pl.when(leading)
    def _():
        def nearness(place):
            d, o = place
            return abs(2 * o - rowcount) - rowcount // 2 * d - CX * (o % CX == CX // 2)

        peers = [(d, o) for d in range(groups) for o in range(rowcount) if d or o]
        for d, o in sorted(peers, key=nearness):
            peer = (lax.rem(grp + d, groups), lax.rem(row + o, rowcount))
            pl.semaphore_signal(barrier, inc=1, device_id=peer, device_id_type=MESH)

    loads = [
        pltpu.make_async_copy(source, target, in_sem.at[k])
        for k, (source, target) in enumerate(
            [(links_hbm, links_ref), (coefs_hbm, coefs_ref), (react_hbm, react_ref), (right_hbm, right_ref)]
        )
    ]
    for load in loads:
        load.start()

    lane = lax.broadcasted_iota(jnp.int32, (count, count), 1)
    down = lax.broadcasted_iota(jnp.int32, (count, count), 0)
    same_z = (down // SUB == lane // SUB).astype(jnp.float32)
    spread[0:count] = same_z
    spread[count : 2 * count] = same_z
    low = tile_iota(1)
    element = ((low % CX) * CY + low // CX % CY) * CZ + low // SUB

    def to_lanes(line):
        return jnp.take_along_axis(jnp.broadcast_to(line, (SUB, count)), element, axis=1)[0:1]

    for load in loads[:3]:
        load.wait()
    slots = to_lanes(links_ref[0:1, :] - me * count)
    order[...] = (down == slots).astype(jnp.float32)
    mass = to_lanes(coefs_ref[...] * (-1.0 / 12.0))
    react = thirds(react_ref[...])
    react = jnp.concatenate(react + [jnp.zeros((SUB - 3, count), jnp.float32)], axis=0)
    loads[3].wait()
    stack = jnp.concatenate([react] + thirds(right_ref[...]), axis=0)
    stack = jnp.dot(stack, order[...], preferred_element_type=jnp.float32)
    react = added([stack[k : k + 1] for k in range(3)])
    auxout[...] = jnp.concatenate([mass, react], axis=0)
    field = added([stack[SUB + k * nrhs : SUB + (k + 1) * nrhs] for k in range(3)])

    def post(t, source, target, send, recv):
        return pltpu.make_async_remote_copy(
            src_ref=source(t), dst_ref=target.at[me], send_sem=send.at[t], recv_sem=recv,
            device_id=leader(t), device_id_type=MESH,
        )

    def post_aux(t):
        return post(t, lambda t: auxout, auxin, aux_send, aux_recv.at[me])

    def post_field(t):
        return post(t, lambda t: outbox.at[t], inbox, out_send, out_recv.at[me])

    def each_post(act):
        for send in (post_aux, post_field):

            @pl.when(leading)
            def _(send=send):
                for k in range(leaders - 1):
                    act(send(another(k)))

            @pl.when(jnp.logical_not(leading))
            def _(send=send):
                for t in range(leaders):
                    act(send(t))

    for t in range(leaders):
        outbox[t] = exchanged(field[t * SUB : (t + 1) * SUB])
    pl.semaphore_wait(barrier, jnp.where(leading, leaders - 1, leaders))

    each_post(lambda copy: copy.start())

    def reply(b):
        return pltpu.make_async_remote_copy(
            src_ref=solved.at[b], dst_ref=answers.at[rank],
            send_sem=back_send.at[b], recv_sem=back_recv.at[rank],
            device_id=block(b), device_id_type=MESH,
        )

    outside = [
        (g, r) for r in range(rowcount) for g in range(groups) if r >= (near, second)[g]
    ]

    @pl.when(leading)
    def _():
        def arrived(b, source, target, send, recv):
            pltpu.make_async_remote_copy(
                src_ref=source, dst_ref=target.at[b], send_sem=send.at[0], recv_sem=recv.at[b],
                device_id=block(b), device_id_type=MESH,
            ).wait_recv()

        def await_rows(part, source, target, send, recv):
            if part == 0:
                for k in range(leaders - 1):
                    arrived(place_of(another(k)), source, target, send, recv)
            for g, r in outside:
                if r * 2 // rowcount == part:
                    arrived(g * rowcount + r, source, target, send, recv)

        own = tile_iota(1) % SUB == tile_iota(0)
        half = rowcount // 2

        def expand(part):
            rows = [(k, p * rowcount + part * half) for k in range(2) for p in range(groups)]
            for at, (k, begin) in enumerate(rows):
                high, middle, _ = thirds(auxin[begin : begin + half, k, :])
                wide[0, at * half : (at + 1) * half] = high
                wide[1, at * half : (at + 1) * half] = middle
            pieces = [
                jnp.concatenate(
                    [
                        jnp.where(own, wide[which, k : k + 1, :], 0.0)
                        for k in range(len(rows) * half)
                    ],
                    axis=0,
                )
                for which in range(2)
            ]
            tiles = jnp.dot(
                jnp.concatenate(pieces, axis=1), spread[...], preferred_element_type=jnp.float32
            )
            tiles = [tiles[k * SUB : (k + 1) * SUB] for k in range(len(rows) * half)]
            for q in range(half):
                for k, m in enumerate(paired(tiles[q], tiles[half + q])):
                    y = CY * (part * half + q) + k
                    m_z = turned(m, SUB)
                    low, low_z = turned(m, 1, 0), turned(m_z, 1, 0)
                    masses[y], masses_z[y] = m, m_z
                    lows[y], lows_z[y] = low, low_z
                    boths[y], boths_z[y] = m + low, m_z + low_z
                for k, react in enumerate(paired(tiles[2 * half + q], tiles[3 * half + q])):
                    diag[CY * (part * half + q) + k] = react

        def settle(ys):
            for y in ys:
                z = (y - 1) % planes
                diag[y] = diag[y] - 4.0 * ((boths[y] + boths_z[y]) + (boths[z] + boths_z[z]))

        def take_in(part):
            for q in range(part * half, (part + 1) * half):
                for k, value in enumerate(paired(inbox[q], inbox[rowcount + q])):
                    bases[0, CY * q + k] = value

        def apply_operator(source, sink, ys=None, taken=None):
            taken = {} if taken is None else taken

            def around(y):
                y = y % planes
                if y not in taken:
                    v = source(y)
                    above, below = turned(v, -SUB), turned(v, SUB)
                    taken[y] = (v, above, below, v + above, v + below)
                return taken[y]

            for y in range(planes) if ys is None else ys:
                v, above, below, _, _ = around(y)
                _, next_above, next_below, next_up, next_down = around(y + 1)
                _, last_above, last_below, last_up, last_down = around(y - 1)
                sides = [above + next_up, below + next_down, above + last_up, below + last_down]
                diagonal = [next_above, next_below, last_above, last_below]

                def weighed(a, b, values, y=y):
                    z = (y - 1) % planes
                    products = [
                        c * value for c, value in zip((a[y], b[y], a[z], b[z]), values)
                    ]
                    return (products[0] + products[1]) + (products[2] + products[3])

                ahead = turned(weighed(lows, lows_z, sides), -1, 0)
                behind = turned(weighed(masses, masses_z, sides), 1, 0)
                middle = weighed(boths, boths_z, diagonal) + diag[y] * v
                sink(y, middle + (ahead + behind))

        square, cross = Total(), Total()

        def first_image(y, image):
            powers[0, y] = image
            square.add(image * image)
            cross.add(bases[0, y] * image)

        taken = {}
        early = range(1, planes // 2 - 1)
        late = list(range(planes // 2 - 1, planes)) + [0]
        for part, ready, ys in ((0, range(1, planes // 2), early), (1, list(range(planes // 2, planes)) + [0], late)):
            if part == 0:
                auxin[me] = auxout[...]
                inbox[me] = outbox[rank]
            await_rows(part, auxout, auxin, aux_send, aux_recv)
            expand(part)
            settle(ready)
            await_rows(part, outbox.at[0], inbox, out_send, out_recv)
            take_in(part)
            apply_operator(lambda y: bases[0, y], first_image, ys, taken)
        def stored(sweep, k):
            def sink(y, image):
                powers[sweep * DEGREE + k, y] = image

            return sink

        def mixed(factors, terms):
            value = factors[0] * terms[0]
            for factor, term in zip(factors[1:], terms[1:]):
                value = value + factor * term
            return value

        apply_operator(lambda y: powers[0, y], stored(0, 1))
        square, cross = summed(square, cross)
        inverse = cross / square
        scales = [inverse]
        for _ in range(DEGREE - 1):
            scales.append(scales[-1] * inverse)
        corrects, differs = chebyshev_weights()
        corrects = [b * scale for b, scale in zip(corrects, scales)]
        differs = [c * scale for c, scale in zip(differs, scales)]

        def closing(sweep, along, length):
            def sink(y, image):
                begin = sweep * DEGREE
                terms = [powers[begin + k, y] for k in range(DEGREE - 1)]
                start = bases[sweep, y]
                change = mixed(differs, terms + [image])
                along.add(start * change)
                length.add(change * change)
                changes[y] = change
                corrections[sweep, y] = mixed(corrects, [start] + terms)

            return sink

        apply_operator(lambda y: powers[1, y], stored(0, 2))
        along, length = Total(), Total()
        apply_operator(lambda y: powers[2, y], closing(0, along, length))
        apply_operator(lambda y: changes[y], stored(0, 3))
        along, length = summed(along, length)
        omega = along / length
        begin = Total()

        def second_start(y):
            base = bases[0, y] - omega * changes[y]
            bases[1, y] = base
            begin.add(base * base)
            image = powers[0, y] - omega * powers[3, y]
            powers[DEGREE, y] = image
            return image

        apply_operator(second_start, stored(1, 1))
        began = over_z(begin.folded())
        apply_operator(lambda y: powers[DEGREE + 1, y], stored(1, 2))
        along, length = Total(), Total()
        apply_operator(lambda y: powers[DEGREE + 2, y], closing(1, along, length))
        for q in range(rowcount):
            for sweep in range(SWEEPS):
                halves = [corrections[sweep, CY * q + k] for k in range(CY)]
                if sweep == 0:
                    halves = [omega * value for value in halves]
                for p, tile in enumerate(paired(*halves)):
                    mixes[sweep, p * rowcount + q] = tile
        along, length = summed(along, length)
        omega = along / length
        group = tile_iota(1) // SUB
        last = jnp.maximum(began - omega * along, 0.0)
        rms = jnp.where(group == rank, began, jnp.where(group == rank + leaders, last, 0.0))
        rms = jnp.sqrt(rms / total)[0:1]
        for b in range(blocks):
            solved[b, 0:SUB] = mixes[0, b] + omega * mixes[1, b]
            solved[b, SUB : SUB + 1] = rms
        for k in range(leaders - 1):
            reply(place_of(another(k))).start()
        for g, r in outside:
            reply(g * rowcount + r).start()
        answers[rank] = solved[me]

    def await_reply(t):
        pltpu.make_async_remote_copy(
            src_ref=solved.at[0], dst_ref=answers.at[t],
            send_sem=back_send.at[0], recv_sem=back_recv.at[t],
            device_id=leader(t), device_id_type=MESH,
        ).wait_recv()

    @pl.when(leading)
    def _():
        for k in range(leaders - 1):
            await_reply(another(k))

    @pl.when(jnp.logical_not(leading))
    def _():
        for t in range(leaders):
            await_reply(t)

    whole = jnp.concatenate([exchanged(answers[t, 0:SUB]) for t in range(leaders)], axis=0)
    whole = jnp.concatenate(thirds(whole), axis=0)
    whole = lax.dot_general(
        whole, order[...], (((1,), (1,)), ((), ())), preferred_element_type=jnp.float32
    )
    solution_ref[...] = added([whole[k * nrhs : (k + 1) * nrhs] for k in range(3)])
    line = answers[0, SUB : SUB + 1]
    for t in range(1, leaders):
        line = line + answers[t, SUB : SUB + 1]
    other = turned(line, count // 2)
    rms_ref[...] = jnp.concatenate([line, other], axis=0)[:, :nrhs]

    each_post(lambda copy: copy.wait_send())

    @pl.when(leading)
    def _():
        for o in range(1, blocks):
            reply(lax.rem(me + o, blocks)).wait_send()


def write_out(solution_ref, rms_ref, out_hbm, rms_hbm, sems):
    copies = [
        pltpu.make_async_copy(solution_ref, out_hbm, sems.at[0]),
        pltpu.make_async_copy(rms_ref, rms_hbm, sems.at[1]),
    ]
    for copy in copies:
        copy.start()
    for copy in copies:
        copy.wait()


def whole_sweeps(groups, rowcount, right_side, links, coefs, reaction):
    nrhs, count = right_side.shape
    leaders = nrhs // SUB
    blocks = groups * rowcount
    planes = rowcount * CY
    dma = pltpu.SemaphoreType.DMA
    vmem = pl.BlockSpec(memory_space=pltpu.VMEM)

    def space(*shape):
        return pltpu.VMEM(shape, jnp.float32)

    plane = space(planes, SUB, count)
    twice = space(SWEEPS, planes, SUB, count)
    found = pl.pallas_call(
        functools.partial(kernel, groups, rowcount, count * groups * rowcount),
        out_shape=(pltpu.VMEM((nrhs, count), jnp.float32), pltpu.VMEM((SWEEPS, nrhs), jnp.float32)),
        in_specs=[pl.BlockSpec(memory_space=pl.ANY)] * 4,
        out_specs=(vmem, vmem),
        scratch_shapes=[
            space(nrhs, count), pltpu.VMEM(links.shape, jnp.int32), space(1, count), space(1, count),
            space(2, count), space(blocks, 2, count),
            space(leaders, SUB, count), space(blocks, SUB, count),
            space(leaders, SUB + 1, count), space(blocks, SUB + 1, count),
            space(count, count), space(2 * count, count), space(2, 2 * blocks, count),
            plane, plane, plane, plane, plane, plane, plane,
            twice, plane, twice, space(SWEEPS * DEGREE, planes, SUB, count),
            space(SWEEPS, blocks, SUB, count),
            dma((4,)), dma((leaders,)), dma((blocks,)), dma((leaders,)), dma((blocks,)),
            dma((blocks,)), dma((leaders,)),
        ],
        compiler_params=pltpu.CompilerParams(collective_id=0, has_side_effects=True),
    )(right_side, links, coefs.reshape(1, count), reaction.reshape(1, count))
    return pl.pallas_call(
        write_out,
        out_shape=(
            jax.ShapeDtypeStruct((nrhs, count), jnp.float32),
            jax.ShapeDtypeStruct((SWEEPS, nrhs), jnp.float32),
        ),
        in_specs=[vmem, vmem],
        out_specs=[pl.BlockSpec(memory_space=pl.ANY)] * 2,
        scratch_shapes=[dma((2,))],
    )(*[pltpu.with_memory_space_constraint(f, pltpu.VMEM) for f in found])


def in_one_kernel(mesh):
    return mesh.shape["grp"] == SUB // CX and 2 * SUB <= mesh.shape["row"] <= 4 * SUB


def solution(mesh):
    body = on_device
    if in_one_kernel(mesh):
        body = functools.partial(whole_sweeps, mesh.shape["grp"], mesh.shape["row"])
    return jax.shard_map(
        body,
        mesh=mesh,
        in_specs=(
            P(None, ("grp", "row")),
            P(None, ("grp", "row")),
            P(("grp", "row")),
            P(("grp", "row")),
        ),
        out_specs=(P(None, ("grp", "row")), P()),
        check_vma=False,
    )
```

```python
import functools
import math

import jax
import jax.numpy as jnp
import numpy as np
from jax import lax
from jax.experimental import pallas as pl
from jax.experimental.pallas import tpu as pltpu
from jax.sharding import PartitionSpec as P

SWEEPS = 2
DEGREE = 4
CX, CY, CZ = 4, 2, 16
SUB, LANES = 8, 128
MESH = pl.DeviceIdType.MESH
HIGHEST = lax.Precision.HIGHEST


def shifted(block, axis, distance):
    devices = range(lax.axis_size(axis))
    route = [((i - distance) % len(devices), i) for i in devices]
    return lax.ppermute(block, axis, route)


def element_matrix():
    node_ids = np.arange(8)
    corner = np.stack([node_ids % 2, node_ids // 2 % 2, node_ids // 4], axis=1)
    gauss_points = np.array([0.5 - 0.5 / math.sqrt(3.0), 0.5 + 0.5 / math.sqrt(3.0)])
    stiffness = np.zeros((8, 8))
    for q in range(8):
        quad_point = gauss_points[np.array([q % 2, q // 2 % 2, q // 4])]
        values = np.where(corner > 0.5, quad_point, 1.0 - quad_point)
        slopes = np.where(corner > 0.5, 1.0, -1.0)
        gradient = np.stack(
            [
                slopes[:, 0] * values[:, 1] * values[:, 2],
                values[:, 0] * slopes[:, 1] * values[:, 2],
                values[:, 0] * values[:, 1] * slopes[:, 2],
            ],
            axis=1,
        )
        stiffness = stiffness + gradient @ gradient.T / 8.0
    return stiffness


def element_images(window, offsets, weights, stiffness):
    corners = window[:, offsets]
    images = (
        jnp.einsum("ml,rle->rme", stiffness, corners, precision=lax.Precision.HIGHEST) * weights
    )
    return jnp.zeros_like(window).at[:, offsets].add(images)


def on_device(right_side, links, coefs, reaction):
    stiffness = jnp.asarray(element_matrix(), dtype=jnp.float32)
    count = right_side.shape[1]
    groups = lax.axis_size("grp")
    rowcount = lax.axis_size("row")
    group_id = lax.axis_index("grp")
    row_id = lax.axis_index("row")
    total = count * groups * rowcount
    owner = links // count
    slot = links % count
    first = jnp.mod(owner // rowcount - group_id, groups)
    second = jnp.mod(owner % rowcount - row_id, rowcount)
    offsets = (first * 2 + second) * count + slot

    def apply_operator(field):
        above_row = shifted(field, "row", -1)
        upper = shifted(jnp.stack([field, above_row], axis=0), "grp", -1)
        window = jnp.concatenate([field, above_row, upper[0], upper[1]], axis=1)
        summed = element_images(window, offsets, coefs, stiffness)
        back = shifted(
            jnp.stack([summed[:, 2 * count : 3 * count], summed[:, 3 * count :]], axis=0), "grp", 1
        )
        first_col = summed[:, :count] + back[0]
        second_col = summed[:, count : 2 * count] + back[1]
        first_col = first_col + shifted(second_col, "row", 1)
        return first_col + reaction * field

    image = apply_operator(right_side)
    cross, square = lax.psum(
        (jnp.sum(right_side * image, axis=1), jnp.sum(image * image, axis=1)), ("grp", "row")
    )
    theta = square / cross
    upper = (1.5 * theta)[:, None]
    lower = upper / 10.0
    center = (upper + lower) / 2.0
    half = (upper - lower) / 2.0
    sigma = center / half
    solution = jnp.zeros_like(right_side)
    residual = right_side
    history = []
    for sweep in range(SWEEPS):
        start = residual
        correction = jnp.zeros_like(right_side)
        rho_now = 1.0 / sigma
        direction = residual / center
        for step in range(DEGREE):
            correction = correction + direction
            residual = residual - apply_operator(direction)
            if step + 1 < DEGREE:
                rho_next = 1.0 / (2.0 * sigma - rho_now)
                direction = rho_next * rho_now * direction + 2.0 * rho_next / half * residual
                rho_now = rho_next
        change = start - residual
        along, length, begin = lax.psum(
            (
                jnp.sum(start * change, axis=1),
                jnp.sum(change * change, axis=1),
                jnp.sum(start * start, axis=1),
            ),
            ("grp", "row"),
        )
        omega = along / length
        residual = start - omega[:, None] * change
        squares = begin - 2.0 * omega * along + omega * omega * length
        solution = solution + omega[:, None] * correction
        history.append(jnp.sqrt(squares / total))
    return (solution, jnp.stack(history, axis=0))


def thirds(a):
    high = a.astype(jnp.bfloat16).astype(jnp.float32)
    rest = a - high
    middle = rest.astype(jnp.bfloat16).astype(jnp.float32)
    return [high, middle, rest - middle]


def added(parts):
    high, middle, low = parts
    return high + middle + low


def turned(a, distance, axis=1):
    return pltpu.roll(a, distance % a.shape[axis], axis)


def tile_iota(axis):
    return lax.broadcasted_iota(jnp.int32, (SUB, LANES), axis)


def exchanged(tile):
    sub, low = tile_iota(0), tile_iota(1)
    for unit, radix in ((1, 4), (4, 2)):
        ahead = low // unit % radix - sub // unit % radix
        result = tile
        for k in range(1 - radix, radix):
            if k:
                moved = turned(turned(tile, -k * unit, 0), k * unit)
                result = jnp.where(ahead == k, moved, result)
        tile = result
    return tile


def paired(first, second):
    top = tile_iota(0) < SUB // 2
    return (
        jnp.where(top, first, turned(second, SUB // 2, 0)),
        jnp.where(top, turned(first, SUB // 2, 0), second),
    )


def chebyshev_weights():
    center, half = (1.5 + 0.15) / 2.0, (1.5 - 0.15) / 2.0
    sigma = center / half
    rho_now = 1.0 / sigma
    direction, residual = np.zeros(DEGREE + 1), np.zeros(DEGREE + 1)
    correction = np.zeros(DEGREE + 1)
    residual[0], direction[0] = 1.0, 1.0 / center
    for _ in range(DEGREE):
        correction = correction + direction
        residual = residual - np.roll(direction, 1)
        rho_next = 1.0 / (2.0 * sigma - rho_now)
        direction = rho_next * rho_now * direction + 2.0 * rho_next / half * residual
        rho_now = rho_next
    return [float(b) for b in correction[:DEGREE]], [-float(c) for c in residual[1:]]


class Total:
    def __init__(self):
        self.parts = [None] * 4
        self.at = 0

    def add(self, value):
        k = self.at % 4
        self.parts[k] = value if self.parts[k] is None else self.parts[k] + value
        self.at += 1

    def folded(self):
        a, b, c, d = self.parts
        value = (a + b) + (c + d)
        for bit in (4, 2, 1):
            value = value + turned(value, bit, 0)
        return value


def over_z(value):
    parts = [value] + [turned(value, SUB * k) for k in range(1, LANES // SUB)]
    while len(parts) > 1:
        parts = [a + b for a, b in zip(parts[::2], parts[1::2])]
    return parts[0]


def summed(first, second):
    top = tile_iota(0) < SUB // 2
    both = over_z(jnp.where(top, first.folded(), second.folded()))
    other = turned(both, SUB // 2, 0)
    return jnp.where(top, both, other), jnp.where(top, other, both)


def kernel(
    groups, rowcount, total,
    right_hbm, links_hbm, coefs_hbm, react_hbm,
    solution_ref, rms_ref,
    right_ref, links_ref, coefs_ref, react_ref,
    auxout, auxin, outbox, inbox, answers, solved, order, spread, wide,
    masses, masses_z, lows, lows_z, boths, boths_z, diag,
    bases, changes, corrections, powers, mixes,
    in_sem, aux_send, aux_recv, out_send, out_recv, back_send, back_recv,
):
    nrhs, count = right_ref.shape
    leaders = nrhs // SUB
    near, second = leaders - CY, CY
    blocks = groups * rowcount
    planes = rowcount * CY
    grp = lax.axis_index("grp")
    row = lax.axis_index("row")
    me = grp * rowcount + row
    leading = row < jnp.where(grp == 0, near, second)
    rank = jnp.where(grp == 0, row, near + row)

    def leader(t):
        if isinstance(t, int):
            return (0, t) if t < near else (1, t - near)
        return (jnp.where(t < near, 0, 1), jnp.where(t < near, t, t - near))

    def block(b):
        return (b // rowcount, lax.rem(b, rowcount))

    def place_of(t):
        return jnp.where(t < near, t, rowcount + t - near)

    def another(k):
        return jnp.where(k < rank, k, k + 1)

    barrier = pltpu.get_barrier_semaphore()

    @pl.when(leading)
    def _():
        def nearness(place):
            d, o = place
            return abs(2 * o - rowcount) - rowcount // 2 * d - CX * (o % CX == CX // 2)

        peers = [(d, o) for d in range(groups) for o in range(rowcount) if d or o]
        for d, o in sorted(peers, key=nearness):
            peer = (lax.rem(grp + d, groups), lax.rem(row + o, rowcount))
            pl.semaphore_signal(barrier, inc=1, device_id=peer, device_id_type=MESH)

    loads = [
        pltpu.make_async_copy(source, target, in_sem.at[k])
        for k, (source, target) in enumerate(
            [(links_hbm, links_ref), (coefs_hbm, coefs_ref), (react_hbm, react_ref), (right_hbm, right_ref)]
        )
    ]
    for load in loads:
        load.start()

    lane = lax.broadcasted_iota(jnp.int32, (count, count), 1)
    down = lax.broadcasted_iota(jnp.int32, (count, count), 0)
    same_z = (down // SUB == lane // SUB).astype(jnp.float32)
    spread[0:count] = same_z
    spread[count : 2 * count] = same_z
    low = tile_iota(1)
    element = ((low % CX) * CY + low // CX % CY) * CZ + low // SUB

    def to_lanes(line):
        return jnp.take_along_axis(jnp.broadcast_to(line, (SUB, count)), element, axis=1)[0:1]

    for load in loads[:3]:
        load.wait()
    slots = to_lanes(links_ref[0:1, :] - me * count)
    order[...] = (down == slots).astype(jnp.float32)
    mass = to_lanes(coefs_ref[...] * (-1.0 / 12.0))
    react = thirds(react_ref[...])
    react = jnp.concatenate(react + [jnp.zeros((SUB - 3, count), jnp.float32)], axis=0)
    loads[3].wait()
    stack = jnp.concatenate([react] + thirds(right_ref[...]), axis=0)
    stack = jnp.dot(stack, order[...], preferred_element_type=jnp.float32)
    react = added([stack[k : k + 1] for k in range(3)])
    auxout[...] = jnp.concatenate([mass, react], axis=0)
    field = added([stack[SUB + k * nrhs : SUB + (k + 1) * nrhs] for k in range(3)])

    own_part = jnp.where(row < rowcount // 2, 0, 1)

    def post(t, source, target, send, recv):
        return pltpu.make_async_remote_copy(
            src_ref=source(t), dst_ref=target.at[me], send_sem=send, recv_sem=recv,
            device_id=leader(t), device_id_type=MESH,
        )

    def post_aux(t):
        return post(t, lambda t: auxout, auxin, aux_send, aux_recv.at[own_part])

    def post_field(t):
        return post(t, lambda t: outbox.at[t], inbox, out_send, out_recv.at[own_part])

    def start_posts():
        for send in (post_aux, post_field):

            @pl.when(leading)
            def _(send=send):
                for k in range(leaders - 1):
                    send(another(k)).start()

            @pl.when(jnp.logical_not(leading))
            def _(send=send):
                for t in range(leaders):
                    send(t).start()

    def whole_of(ref, number, send, recv):
        return pltpu.make_async_remote_copy(
            src_ref=ref.at[pl.ds(0, number)], dst_ref=ref.at[pl.ds(0, number)],
            send_sem=send, recv_sem=recv, device_id=leader(0), device_id_type=MESH,
        )

    def sent_posts(number):
        whole_of(auxin, number, aux_send, aux_recv.at[0]).wait_send()
        whole_of(inbox, number, out_send, out_recv.at[0]).wait_send()

    for t in range(leaders):
        outbox[t] = exchanged(field[t * SUB : (t + 1) * SUB])
    pl.semaphore_wait(barrier, jnp.where(leading, leaders - 1, leaders))

    start_posts()

    def reply(b):
        return pltpu.make_async_remote_copy(
            src_ref=solved.at[b], dst_ref=answers.at[rank],
            send_sem=back_send, recv_sem=back_recv,
            device_id=block(b), device_id_type=MESH,
        )

    outside = [
        (g, r) for r in range(rowcount) for g in range(groups) if r >= (near, second)[g]
    ]

    @pl.when(leading)
    def _():
        def await_rows(part, target, send, recv):
            whole_of(target, blocks // 2 - 1 + part, send, recv.at[part]).wait_recv()

        own = tile_iota(1) % SUB == tile_iota(0)
        half = rowcount // 2

        def expand(part):
            rows = [(k, p * rowcount + part * half) for k in range(2) for p in range(groups)]
            for at, (k, begin) in enumerate(rows):
                high, middle, _ = thirds(auxin[begin : begin + half, k, :])
                wide[0, at * half : (at + 1) * half] = high
                wide[1, at * half : (at + 1) * half] = middle
            pieces = [
                jnp.concatenate(
                    [
                        jnp.where(own, wide[which, k : k + 1, :], 0.0)
                        for k in range(len(rows) * half)
                    ],
                    axis=0,
                )
                for which in range(2)
            ]
            tiles = jnp.dot(
                jnp.concatenate(pieces, axis=1), spread[...], preferred_element_type=jnp.float32
            )
            tiles = [tiles[k * SUB : (k + 1) * SUB] for k in range(len(rows) * half)]
            for q in range(half):
                for k, m in enumerate(paired(tiles[q], tiles[half + q])):
                    y = CY * (part * half + q) + k
                    m_z = turned(m, SUB)
                    low, low_z = turned(m, 1, 0), turned(m_z, 1, 0)
                    masses[y], masses_z[y] = m, m_z
                    lows[y], lows_z[y] = low, low_z
                    boths[y], boths_z[y] = m + low, m_z + low_z
                for k, react in enumerate(paired(tiles[2 * half + q], tiles[3 * half + q])):
                    diag[CY * (part * half + q) + k] = react

        def settle(ys):
            for y in ys:
                z = (y - 1) % planes
                diag[y] = diag[y] - 4.0 * ((boths[y] + boths_z[y]) + (boths[z] + boths_z[z]))

        def take_in(part):
            for q in range(part * half, (part + 1) * half):
                for k, value in enumerate(paired(inbox[q], inbox[rowcount + q])):
                    bases[0, CY * q + k] = value

        def apply_operator(source, sink, ys=None, taken=None):
            taken = {} if taken is None else taken

            def around(y):
                y = y % planes
                if y not in taken:
                    v = source(y)
                    above, below = turned(v, -SUB), turned(v, SUB)
                    taken[y] = (v, above, below, v + above, v + below)
                return taken[y]

            for y in range(planes) if ys is None else ys:
                v, above, below, _, _ = around(y)
                _, next_above, next_below, next_up, next_down = around(y + 1)
                _, last_above, last_below, last_up, last_down = around(y - 1)
                sides = [above + next_up, below + next_down, above + last_up, below + last_down]
                diagonal = [next_above, next_below, last_above, last_below]

                def weighed(a, b, values, y=y):
                    z = (y - 1) % planes
                    products = [
                        c * value for c, value in zip((a[y], b[y], a[z], b[z]), values)
                    ]
                    return (products[0] + products[1]) + (products[2] + products[3])

                ahead = turned(weighed(lows, lows_z, sides), -1, 0)
                behind = turned(weighed(masses, masses_z, sides), 1, 0)
                middle = weighed(boths, boths_z, diagonal) + diag[y] * v
                sink(y, middle + (ahead + behind))

        square, cross = Total(), Total()

        def first_image(y, image):
            powers[0, y] = image
            square.add(image * image)
            cross.add(bases[0, y] * image)

        taken = {}
        early = range(1, planes // 2 - 1)
        late = list(range(planes // 2 - 1, planes)) + [0]
        for part, ready, ys in ((0, range(1, planes // 2), early), (1, list(range(planes // 2, planes)) + [0], late)):
            if part == 0:
                auxin[me] = auxout[...]
                inbox[me] = outbox[rank]
            await_rows(part, auxin, aux_send, aux_recv)
            expand(part)
            settle(ready)
            await_rows(part, inbox, out_send, out_recv)
            take_in(part)
            apply_operator(lambda y: bases[0, y], first_image, ys, taken)
        def stored(sweep, k):
            def sink(y, image):
                powers[sweep * DEGREE + k, y] = image

            return sink

        def mixed(factors, terms):
            value = factors[0] * terms[0]
            for factor, term in zip(factors[1:], terms[1:]):
                value = value + factor * term
            return value

        apply_operator(lambda y: powers[0, y], stored(0, 1))
        square, cross = summed(square, cross)
        inverse = cross / square
        scales = [inverse]
        for _ in range(DEGREE - 1):
            scales.append(scales[-1] * inverse)
        corrects, differs = chebyshev_weights()
        corrects = [b * scale for b, scale in zip(corrects, scales)]
        differs = [c * scale for c, scale in zip(differs, scales)]

        def closing(sweep, along, length):
            def sink(y, image):
                begin = sweep * DEGREE
                terms = [powers[begin + k, y] for k in range(DEGREE - 1)]
                start = bases[sweep, y]
                change = mixed(differs, terms + [image])
                along.add(start * change)
                length.add(change * change)
                changes[y] = change
                corrections[sweep, y] = mixed(corrects, [start] + terms)

            return sink

        apply_operator(lambda y: powers[1, y], stored(0, 2))
        along, length = Total(), Total()
        apply_operator(lambda y: powers[2, y], closing(0, along, length))
        apply_operator(lambda y: changes[y], stored(0, 3))
        along, length = summed(along, length)
        omega = along / length
        begin = Total()

        def second_start(y):
            base = bases[0, y] - omega * changes[y]
            bases[1, y] = base
            begin.add(base * base)
            image = powers[0, y] - omega * powers[3, y]
            powers[DEGREE, y] = image
            return image

        apply_operator(second_start, stored(1, 1))
        began = over_z(begin.folded())
        apply_operator(lambda y: powers[DEGREE + 1, y], stored(1, 2))
        along, length = Total(), Total()
        apply_operator(lambda y: powers[DEGREE + 2, y], closing(1, along, length))
        for q in range(rowcount):
            for sweep in range(SWEEPS):
                halves = [corrections[sweep, CY * q + k] for k in range(CY)]
                if sweep == 0:
                    halves = [omega * value for value in halves]
                for p, tile in enumerate(paired(*halves)):
                    mixes[sweep, p * rowcount + q] = tile
        along, length = summed(along, length)
        omega = along / length
        group = tile_iota(1) // SUB
        last = jnp.maximum(began - omega * along, 0.0)
        rms = jnp.where(group == rank, began, jnp.where(group == rank + leaders, last, 0.0))
        rms = jnp.sqrt(rms / total)[0:1]
        for b in range(blocks):
            solved[b, 0:SUB] = mixes[0, b] + omega * mixes[1, b]
            solved[b, SUB : SUB + 1] = rms
        for k in range(leaders - 1):
            reply(place_of(another(k))).start()
        for g, r in outside:
            reply(g * rowcount + r).start()
        answers[rank] = solved[me]

    def answered(number):
        whole_of(answers, number, back_send, back_recv).wait_recv()

    @pl.when(leading)
    def _():
        answered(leaders - 1)

    @pl.when(jnp.logical_not(leading))
    def _():
        answered(leaders)

    whole = jnp.concatenate([exchanged(answers[t, 0:SUB]) for t in range(leaders)], axis=0)
    whole = jnp.concatenate(thirds(whole), axis=0)
    whole = lax.dot_general(
        whole, order[...], (((1,), (1,)), ((), ())), preferred_element_type=jnp.float32
    )
    solution_ref[...] = added([whole[k * nrhs : (k + 1) * nrhs] for k in range(3)])
    line = answers[0, SUB : SUB + 1]
    for t in range(1, leaders):
        line = line + answers[t, SUB : SUB + 1]
    other = turned(line, count // 2)
    rms_ref[...] = jnp.concatenate([line, other], axis=0)[:, :nrhs]

    @pl.when(leading)
    def _():
        sent_posts(leaders - 1)
        whole_of(solved, blocks - 1, back_send, back_recv).wait_send()

    @pl.when(jnp.logical_not(leading))
    def _():
        sent_posts(leaders)


def write_out(solution_ref, rms_ref, out_hbm, rms_hbm, sems):
    copies = [
        pltpu.make_async_copy(solution_ref, out_hbm, sems.at[0]),
        pltpu.make_async_copy(rms_ref, rms_hbm, sems.at[1]),
    ]
    for copy in copies:
        copy.start()
    for copy in copies:
        copy.wait()


def whole_sweeps(groups, rowcount, right_side, links, coefs, reaction):
    nrhs, count = right_side.shape
    leaders = nrhs // SUB
    blocks = groups * rowcount
    planes = rowcount * CY
    dma = pltpu.SemaphoreType.DMA
    vmem = pl.BlockSpec(memory_space=pltpu.VMEM)

    def space(*shape):
        return pltpu.VMEM(shape, jnp.float32)

    plane = space(planes, SUB, count)
    twice = space(SWEEPS, planes, SUB, count)
    found = pl.pallas_call(
        functools.partial(kernel, groups, rowcount, count * groups * rowcount),
        out_shape=(pltpu.VMEM((nrhs, count), jnp.float32), pltpu.VMEM((SWEEPS, nrhs), jnp.float32)),
        in_specs=[pl.BlockSpec(memory_space=pl.ANY)] * 4,
        out_specs=(vmem, vmem),
        scratch_shapes=[
            space(nrhs, count), pltpu.VMEM(links.shape, jnp.int32), space(1, count), space(1, count),
            space(2, count), space(blocks, 2, count),
            space(leaders, SUB, count), space(blocks, SUB, count),
            space(leaders, SUB + 1, count), space(blocks, SUB + 1, count),
            space(count, count), space(2 * count, count), space(2, 2 * blocks, count),
            plane, plane, plane, plane, plane, plane, plane,
            twice, plane, twice, space(SWEEPS * DEGREE, planes, SUB, count),
            space(SWEEPS, blocks, SUB, count),
            dma((4,)), dma, dma((2,)), dma, dma((2,)), dma, dma,
        ],
        compiler_params=pltpu.CompilerParams(collective_id=0, has_side_effects=True),
    )(right_side, links, coefs.reshape(1, count), reaction.reshape(1, count))
    return pl.pallas_call(
        write_out,
        out_shape=(
            jax.ShapeDtypeStruct((nrhs, count), jnp.float32),
            jax.ShapeDtypeStruct((SWEEPS, nrhs), jnp.float32),
        ),
        in_specs=[vmem, vmem],
        out_specs=[pl.BlockSpec(memory_space=pl.ANY)] * 2,
        scratch_shapes=[dma((2,))],
    )(*[pltpu.with_memory_space_constraint(f, pltpu.VMEM) for f in found])


def in_one_kernel(mesh):
    return mesh.shape["grp"] == SUB // CX and 2 * SUB <= mesh.shape["row"] <= 4 * SUB


def solution(mesh):
    body = on_device
    if in_one_kernel(mesh):
        body = functools.partial(whole_sweeps, mesh.shape["grp"], mesh.shape["row"])
    return jax.shard_map(
        body,
        mesh=mesh,
        in_specs=(
            P(None, ("grp", "row")),
            P(None, ("grp", "row")),
            P(("grp", "row")),
            P(("grp", "row")),
        ),
        out_specs=(P(None, ("grp", "row")), P()),
        check_vma=False,
    )
```

```python
import functools
import math

import jax
import jax.numpy as jnp
import numpy as np
from jax import lax
from jax.experimental import pallas as pl
from jax.experimental.pallas import tpu as pltpu
from jax.sharding import PartitionSpec as P

SWEEPS = 2
DEGREE = 4
CX, CY, CZ = 4, 2, 16
SUB, LANES = 8, 128
MESH = pl.DeviceIdType.MESH
HIGHEST = lax.Precision.HIGHEST


def shifted(block, axis, distance):
    devices = range(lax.axis_size(axis))
    route = [((i - distance) % len(devices), i) for i in devices]
    return lax.ppermute(block, axis, route)


def element_matrix():
    node_ids = np.arange(8)
    corner = np.stack([node_ids % 2, node_ids // 2 % 2, node_ids // 4], axis=1)
    gauss_points = np.array([0.5 - 0.5 / math.sqrt(3.0), 0.5 + 0.5 / math.sqrt(3.0)])
    stiffness = np.zeros((8, 8))
    for q in range(8):
        quad_point = gauss_points[np.array([q % 2, q // 2 % 2, q // 4])]
        values = np.where(corner > 0.5, quad_point, 1.0 - quad_point)
        slopes = np.where(corner > 0.5, 1.0, -1.0)
        gradient = np.stack(
            [
                slopes[:, 0] * values[:, 1] * values[:, 2],
                values[:, 0] * slopes[:, 1] * values[:, 2],
                values[:, 0] * values[:, 1] * slopes[:, 2],
            ],
            axis=1,
        )
        stiffness = stiffness + gradient @ gradient.T / 8.0
    return stiffness


def element_images(window, offsets, weights, stiffness):
    corners = window[:, offsets]
    images = (
        jnp.einsum("ml,rle->rme", stiffness, corners, precision=lax.Precision.HIGHEST) * weights
    )
    return jnp.zeros_like(window).at[:, offsets].add(images)


def on_device(right_side, links, coefs, reaction):
    stiffness = jnp.asarray(element_matrix(), dtype=jnp.float32)
    count = right_side.shape[1]
    groups = lax.axis_size("grp")
    rowcount = lax.axis_size("row")
    group_id = lax.axis_index("grp")
    row_id = lax.axis_index("row")
    total = count * groups * rowcount
    owner = links // count
    slot = links % count
    first = jnp.mod(owner // rowcount - group_id, groups)
    second = jnp.mod(owner % rowcount - row_id, rowcount)
    offsets = (first * 2 + second) * count + slot

    def apply_operator(field):
        above_row = shifted(field, "row", -1)
        upper = shifted(jnp.stack([field, above_row], axis=0), "grp", -1)
        window = jnp.concatenate([field, above_row, upper[0], upper[1]], axis=1)
        summed = element_images(window, offsets, coefs, stiffness)
        back = shifted(
            jnp.stack([summed[:, 2 * count : 3 * count], summed[:, 3 * count :]], axis=0), "grp", 1
        )
        first_col = summed[:, :count] + back[0]
        second_col = summed[:, count : 2 * count] + back[1]
        first_col = first_col + shifted(second_col, "row", 1)
        return first_col + reaction * field

    image = apply_operator(right_side)
    cross, square = lax.psum(
        (jnp.sum(right_side * image, axis=1), jnp.sum(image * image, axis=1)), ("grp", "row")
    )
    theta = square / cross
    upper = (1.5 * theta)[:, None]
    lower = upper / 10.0
    center = (upper + lower) / 2.0
    half = (upper - lower) / 2.0
    sigma = center / half
    solution = jnp.zeros_like(right_side)
    residual = right_side
    history = []
    for sweep in range(SWEEPS):
        start = residual
        correction = jnp.zeros_like(right_side)
        rho_now = 1.0 / sigma
        direction = residual / center
        for step in range(DEGREE):
            correction = correction + direction
            residual = residual - apply_operator(direction)
            if step + 1 < DEGREE:
                rho_next = 1.0 / (2.0 * sigma - rho_now)
                direction = rho_next * rho_now * direction + 2.0 * rho_next / half * residual
                rho_now = rho_next
        change = start - residual
        along, length, begin = lax.psum(
            (
                jnp.sum(start * change, axis=1),
                jnp.sum(change * change, axis=1),
                jnp.sum(start * start, axis=1),
            ),
            ("grp", "row"),
        )
        omega = along / length
        residual = start - omega[:, None] * change
        squares = begin - 2.0 * omega * along + omega * omega * length
        solution = solution + omega[:, None] * correction
        history.append(jnp.sqrt(squares / total))
    return (solution, jnp.stack(history, axis=0))


def thirds(a):
    high = a.astype(jnp.bfloat16).astype(jnp.float32)
    rest = a - high
    middle = rest.astype(jnp.bfloat16).astype(jnp.float32)
    return [high, middle, rest - middle]


def added(parts):
    high, middle, low = parts
    return high + middle + low


def turned(a, distance, axis=1):
    return pltpu.roll(a, distance % a.shape[axis], axis)


def tile_iota(axis):
    return lax.broadcasted_iota(jnp.int32, (SUB, LANES), axis)


def exchanged(tile):
    sub, low = tile_iota(0), tile_iota(1)
    for unit, radix in ((1, 4), (4, 2)):
        ahead = low // unit % radix - sub // unit % radix
        result = tile
        for k in range(1 - radix, radix):
            if k:
                moved = turned(turned(tile, -k * unit, 0), k * unit)
                result = jnp.where(ahead == k, moved, result)
        tile = result
    return tile


def paired(first, second):
    top = tile_iota(0) < SUB // 2
    return (
        jnp.where(top, first, turned(second, SUB // 2, 0)),
        jnp.where(top, turned(first, SUB // 2, 0), second),
    )


def correction_weights():
    center, half = (1.5 + 0.15) / 2.0, (1.5 - 0.15) / 2.0
    sigma = center / half
    rho_now = 1.0 / sigma
    direction, residual = np.zeros(DEGREE + 1), np.zeros(DEGREE + 1)
    correction = np.zeros(DEGREE + 1)
    residual[0], direction[0] = 1.0, 1.0 / center
    for _ in range(DEGREE):
        correction = correction + direction
        residual = residual - np.roll(direction, 1)
        rho_next = 1.0 / (2.0 * sigma - rho_now)
        direction = rho_next * rho_now * direction + 2.0 * rho_next / half * residual
        rho_now = rho_next
    return [float(b / correction[DEGREE - 1]) for b in correction[: DEGREE - 1]]


class Total:
    def __init__(self):
        self.parts = [None] * 4
        self.at = 0

    def add(self, value):
        k = self.at % 4
        self.parts[k] = value if self.parts[k] is None else self.parts[k] + value
        self.at += 1

    def folded(self):
        a, b, c, d = self.parts
        value = (a + b) + (c + d)
        for bit in (4, 2, 1):
            value = value + turned(value, bit, 0)
        return value


def over_z(value):
    parts = [value] + [turned(value, SUB * k) for k in range(1, LANES // SUB)]
    while len(parts) > 1:
        parts = [a + b for a, b in zip(parts[::2], parts[1::2])]
    return parts[0]


def summed(first, second):
    top = tile_iota(0) < SUB // 2
    both = over_z(jnp.where(top, first.folded(), second.folded()))
    other = turned(both, SUB // 2, 0)
    return jnp.where(top, both, other), jnp.where(top, other, both)


def kernel(
    groups, rowcount, total,
    right_hbm, links_hbm, coefs_hbm, react_hbm,
    solution_ref, rms_ref,
    right_ref, links_ref, coefs_ref, react_ref,
    auxout, auxin, outbox, inbox, answers, solved, order, spread, wide,
    masses, masses_z, flats, flats_z, talls, edges_x, edges_y, edges_z, edges_below, diag,
    bases, changes, corrections, powers, mixes,
    in_sem, aux_send, aux_recv, out_send, out_recv, back_send, back_recv,
):
    nrhs, count = right_ref.shape
    leaders = nrhs // SUB
    near, second = leaders - CY, CY
    blocks = groups * rowcount
    planes = rowcount * CY
    grp = lax.axis_index("grp")
    row = lax.axis_index("row")
    me = grp * rowcount + row
    leading = row < jnp.where(grp == 0, near, second)
    rank = jnp.where(grp == 0, row, near + row)

    def leader(t):
        if isinstance(t, int):
            return (0, t) if t < near else (1, t - near)
        return (jnp.where(t < near, 0, 1), jnp.where(t < near, t, t - near))

    def block(b):
        return (b // rowcount, lax.rem(b, rowcount))

    def place_of(t):
        return jnp.where(t < near, t, rowcount + t - near)

    def another(k):
        return jnp.where(k < rank, k, k + 1)

    barrier = pltpu.get_barrier_semaphore()

    @pl.when(leading)
    def _():
        def nearness(place):
            d, o = place
            return abs(2 * o - rowcount) - rowcount // 2 * d - CX * (o % CX == CX // 2)

        peers = [(d, o) for d in range(groups) for o in range(rowcount) if d or o]
        for d, o in sorted(peers, key=nearness):
            peer = (lax.rem(grp + d, groups), lax.rem(row + o, rowcount))
            pl.semaphore_signal(barrier, inc=1, device_id=peer, device_id_type=MESH)

    loads = [
        pltpu.make_async_copy(source, target, in_sem.at[k])
        for k, (source, target) in enumerate(
            [(links_hbm, links_ref), (coefs_hbm, coefs_ref), (react_hbm, react_ref), (right_hbm, right_ref)]
        )
    ]
    for load in loads:
        load.start()

    lane = lax.broadcasted_iota(jnp.int32, (count, count), 1)
    down = lax.broadcasted_iota(jnp.int32, (count, count), 0)
    same_z = (down // SUB == lane // SUB).astype(jnp.float32)
    spread[0:count] = same_z
    spread[count : 2 * count] = same_z
    low = tile_iota(1)
    element = ((low % CX) * CY + low // CX % CY) * CZ + low // SUB

    def to_lanes(line):
        return jnp.take_along_axis(jnp.broadcast_to(line, (SUB, count)), element, axis=1)[0:1]

    for load in loads[:3]:
        load.wait()
    slots = to_lanes(links_ref[0:1, :] - me * count)
    order[...] = (down == slots).astype(jnp.float32)
    mass = to_lanes(coefs_ref[...] * (1.0 / 12.0))
    react = thirds(react_ref[...])
    react = jnp.concatenate(react + [jnp.zeros((SUB - 3, count), jnp.float32)], axis=0)
    loads[3].wait()
    stack = jnp.concatenate([react] + thirds(right_ref[...]), axis=0)
    stack = jnp.dot(stack, order[...], preferred_element_type=jnp.float32)
    react = added([stack[k : k + 1] for k in range(3)])
    auxout[...] = jnp.concatenate([mass, react], axis=0)
    field = added([stack[SUB + k * nrhs : SUB + (k + 1) * nrhs] for k in range(3)])

    own_part = jnp.where(row < rowcount // 2, 0, 1)

    def post(t, source, target, send, recv):
        return pltpu.make_async_remote_copy(
            src_ref=source(t), dst_ref=target.at[me], send_sem=send, recv_sem=recv,
            device_id=leader(t), device_id_type=MESH,
        )

    def post_aux(t):
        return post(t, lambda t: auxout, auxin, aux_send, aux_recv.at[own_part])

    def post_field(t):
        return post(t, lambda t: outbox.at[t], inbox, out_send, out_recv.at[own_part])

    def start_posts():
        for send in (post_aux, post_field):

            @pl.when(leading)
            def _(send=send):
                for k in range(leaders - 1):
                    send(another(k)).start()

            @pl.when(jnp.logical_not(leading))
            def _(send=send):
                for t in range(leaders):
                    send(t).start()

    def whole_of(ref, number, send, recv):
        return pltpu.make_async_remote_copy(
            src_ref=ref.at[pl.ds(0, number)], dst_ref=ref.at[pl.ds(0, number)],
            send_sem=send, recv_sem=recv, device_id=leader(0), device_id_type=MESH,
        )

    def sent_posts(number):
        whole_of(auxin, number, aux_send, aux_recv.at[0]).wait_send()
        whole_of(inbox, number, out_send, out_recv.at[0]).wait_send()

    for t in range(leaders):
        outbox[t] = exchanged(field[t * SUB : (t + 1) * SUB])
    pl.semaphore_wait(barrier, jnp.where(leading, leaders - 1, leaders))

    start_posts()

    def reply(b):
        return pltpu.make_async_remote_copy(
            src_ref=solved.at[b], dst_ref=answers.at[rank],
            send_sem=back_send, recv_sem=back_recv,
            device_id=block(b), device_id_type=MESH,
        )

    outside = [
        (g, r) for r in range(rowcount) for g in range(groups) if r >= (near, second)[g]
    ]

    @pl.when(leading)
    def _():
        def await_rows(part, target, send, recv):
            whole_of(target, blocks // 2 - 1 + part, send, recv.at[part]).wait_recv()

        own = tile_iota(1) % SUB == tile_iota(0)
        half = rowcount // 2

        def expand(part):
            rows = [(k, p * rowcount + part * half) for k in range(2) for p in range(groups)]
            for at, (k, begin) in enumerate(rows):
                high, middle, _ = thirds(auxin[begin : begin + half, k, :])
                wide[0, at * half : (at + 1) * half] = high
                wide[1, at * half : (at + 1) * half] = middle
            pieces = [
                jnp.concatenate(
                    [
                        jnp.where(own, wide[which, k : k + 1, :], 0.0)
                        for k in range(len(rows) * half)
                    ],
                    axis=0,
                )
                for which in range(2)
            ]
            tiles = jnp.dot(
                jnp.concatenate(pieces, axis=1), spread[...], preferred_element_type=jnp.float32
            )
            tiles = [tiles[k * SUB : (k + 1) * SUB] for k in range(len(rows) * half)]
            for q in range(half):
                for k, m in enumerate(paired(tiles[q], tiles[half + q])):
                    y = CY * (part * half + q) + k
                    m_z = turned(m, SUB)
                    flat, flat_z = m + turned(m, 1, 0), m_z + turned(m_z, 1, 0)
                    masses[y], masses_z[y] = m, m_z
                    flats[y], flats_z[y] = flat, flat_z
                    talls[y], edges_y[y] = m + m_z, flat + flat_z
                for k, react in enumerate(paired(tiles[2 * half + q], tiles[3 * half + q])):
                    diag[CY * (part * half + q) + k] = react

        def settle(ys):
            for y in ys:
                z = (y - 1) % planes
                edges_x[y] = talls[y] + talls[z]
                edges_z[y] = flats[y] + flats[z]
                edges_below[y] = flats_z[y] + flats_z[z]
                diag[y] = diag[y] + 5.0 * (edges_y[y] + edges_y[z])

        def take_in(part):
            for q in range(part * half, (part + 1) * half):
                for k, value in enumerate(paired(inbox[q], inbox[rowcount + q])):
                    bases[0, CY * q + k] = value

        def apply_operator(source, sink, ys):
            taken, pushed = {}, {}

            def around(y):
                y = y % planes
                if y not in taken:
                    v = source(y)
                    above, below = turned(v, -SUB), turned(v, SUB)
                    up, down = v + above, v + below
                    up, down = up + turned(up, -1, 0), down + turned(down, -1, 0)
                    taken[y] = (v, above, below, up, down)
                return taken[y]

            def push(y):
                y = y % planes
                if y not in pushed:
                    (_, _, _, up, down), (_, _, _, next_up, next_down) = around(y), around(y + 1)
                    pushed[y] = masses[y] * (up + next_up) + masses_z[y] * (down + next_down)
                return pushed[y]

            for y in ys:
                v, above, below, _, _ = around(y)
                both = push(y) + push(y - 1)
                edge_x = edges_x[y]
                image = (diag[y] * v + edges_z[y] * above) + edges_below[y] * below
                image = image + (
                    edges_y[y] * around(y + 1)[0] + edges_y[(y - 1) % planes] * around(y - 1)[0]
                )
                image = image + (edge_x * turned(v, -1, 0) - both)
                sink(y, image + turned(edge_x * v - both, 1, 0))

        square, cross = Total(), Total()

        def opening_image(y, image):
            powers[0, y] = image
            square.add(image * image)
            cross.add(bases[0, y] * image)

        def stored(sweep, k):
            def sink(y, image):
                powers[sweep * DEGREE + k, y] = image

            return sink

        def mixed(factors, terms):
            value = factors[0] * terms[0]
            for factor, term in zip(factors[1:], terms[1:]):
                value = value + factor * term
            return value

        def ring(begin):
            return [(begin + k) % planes for k in range(planes)]

        def early(k):
            return range(k, planes // 2 - k)

        def late(k):
            return [y for y in ring(planes // 2 - k) if y not in early(k)]

        def start_plane(y):
            return bases[0, y]

        def first_image(y):
            return powers[0, y]

        auxin[me] = auxout[...]
        inbox[me] = outbox[rank]
        for part, ys in ((0, range(1, planes // 2)), (1, ring(planes // 2)[: planes // 2 + 1])):
            await_rows(part, auxin, aux_send, aux_recv)
            expand(part)
            settle(ys)
            await_rows(part, inbox, out_send, out_recv)
            take_in(part)
            if part == 0:
                apply_operator(start_plane, opening_image, early(1))
                apply_operator(first_image, stored(0, 1), early(2))
                apply_operator(lambda y: powers[1, y], stored(0, 2), early(3))
        apply_operator(start_plane, opening_image, late(1))
        square, cross = summed(square, cross)
        theta = square / cross
        scales = [theta]
        for _ in range(DEGREE - 2):
            scales.append(scales[-1] * theta)
        factors = [b * scale for b, scale in zip(correction_weights(), scales[::-1])]

        def corrected(sweep):
            def source(y):
                begin = sweep * DEGREE
                terms = [bases[sweep, y]] + [powers[begin + k, y] for k in range(DEGREE - 2)]
                value = powers[begin + DEGREE - 2, y] + mixed(factors, terms)
                corrections[sweep, y] = value
                return value

            return source

        def finishing(sweep, along, length):
            def sink(y, change):
                along.add(bases[sweep, y] * change)
                length.add(change * change)
                changes[y] = change

            return sink

        along, length = Total(), Total()
        apply_operator(first_image, stored(0, 1), late(2))
        apply_operator(lambda y: powers[1, y], stored(0, 2), late(3))
        begin_at = planes // 2 - DEGREE + 1
        apply_operator(corrected(0), finishing(0, along, length), ring(begin_at))
        apply_operator(lambda y: changes[y], stored(0, 3), ring(begin_at + 1))
        along, length = summed(along, length)
        omega = along / length
        begin = Total()

        def second_start(y):
            base = bases[0, y] - omega * changes[y]
            bases[1, y] = base
            begin.add(base * base)
            image = powers[0, y] - omega * powers[3, y]
            powers[DEGREE, y] = image
            return image

        apply_operator(second_start, stored(1, 1), ring(begin_at + 2))
        began = over_z(begin.folded())
        apply_operator(lambda y: powers[DEGREE + 1, y], stored(1, 2), ring(begin_at + 3))
        along, length = Total(), Total()
        apply_operator(corrected(1), finishing(1, along, length), ring(begin_at + 4))
        for q in range(rowcount):
            for sweep in range(SWEEPS):
                halves = [corrections[sweep, CY * q + k] for k in range(CY)]
                if sweep == 0:
                    halves = [omega * value for value in halves]
                for p, tile in enumerate(paired(*halves)):
                    mixes[sweep, p * rowcount + q] = tile
        along, length = summed(along, length)
        omega = along / length
        group = tile_iota(1) // SUB
        last = jnp.maximum(began - omega * along, 0.0)
        rms = jnp.where(group == rank, began, jnp.where(group == rank + leaders, last, 0.0))
        rms = jnp.sqrt(rms / total)[0:1]
        for b in range(blocks):
            solved[b, 0:SUB] = mixes[0, b] + omega * mixes[1, b]
            solved[b, SUB : SUB + 1] = rms
        for k in range(leaders - 1):
            reply(place_of(another(k))).start()
        for g, r in outside:
            reply(g * rowcount + r).start()
        answers[rank] = solved[me]

    def answered(number):
        whole_of(answers, number, back_send, back_recv).wait_recv()

    @pl.when(leading)
    def _():
        answered(leaders - 1)

    @pl.when(jnp.logical_not(leading))
    def _():
        answered(leaders)

    whole = jnp.concatenate([exchanged(answers[t, 0:SUB]) for t in range(leaders)], axis=0)
    whole = jnp.concatenate(thirds(whole), axis=0)
    whole = lax.dot_general(
        whole, order[...], (((1,), (1,)), ((), ())), preferred_element_type=jnp.float32
    )
    solution_ref[...] = added([whole[k * nrhs : (k + 1) * nrhs] for k in range(3)])
    line = answers[0, SUB : SUB + 1]
    for t in range(1, leaders):
        line = line + answers[t, SUB : SUB + 1]
    other = turned(line, count // 2)
    rms_ref[...] = jnp.concatenate([line, other], axis=0)[:, :nrhs]

    @pl.when(leading)
    def _():
        sent_posts(leaders - 1)
        whole_of(solved, blocks - 1, back_send, back_recv).wait_send()

    @pl.when(jnp.logical_not(leading))
    def _():
        sent_posts(leaders)


def write_out(solution_ref, rms_ref, out_hbm, rms_hbm, sems):
    copies = [
        pltpu.make_async_copy(solution_ref, out_hbm, sems.at[0]),
        pltpu.make_async_copy(rms_ref, rms_hbm, sems.at[1]),
    ]
    for copy in copies:
        copy.start()
    for copy in copies:
        copy.wait()


def whole_sweeps(groups, rowcount, right_side, links, coefs, reaction):
    nrhs, count = right_side.shape
    leaders = nrhs // SUB
    blocks = groups * rowcount
    planes = rowcount * CY
    dma = pltpu.SemaphoreType.DMA
    vmem = pl.BlockSpec(memory_space=pltpu.VMEM)

    def space(*shape):
        return pltpu.VMEM(shape, jnp.float32)

    plane = space(planes, SUB, count)
    twice = space(SWEEPS, planes, SUB, count)
    found = pl.pallas_call(
        functools.partial(kernel, groups, rowcount, count * groups * rowcount),
        out_shape=(pltpu.VMEM((nrhs, count), jnp.float32), pltpu.VMEM((SWEEPS, nrhs), jnp.float32)),
        in_specs=[pl.BlockSpec(memory_space=pl.ANY)] * 4,
        out_specs=(vmem, vmem),
        scratch_shapes=[
            space(nrhs, count), pltpu.VMEM(links.shape, jnp.int32), space(1, count), space(1, count),
            space(2, count), space(blocks, 2, count),
            space(leaders, SUB, count), space(blocks, SUB, count),
            space(leaders, SUB + 1, count), space(blocks, SUB + 1, count),
            space(count, count), space(2 * count, count), space(2, 2 * blocks, count),
            plane, plane, plane, plane, plane, plane, plane, plane, plane, plane,
            twice, plane, twice, space(SWEEPS * DEGREE, planes, SUB, count),
            space(SWEEPS, blocks, SUB, count),
            dma((4,)), dma, dma((2,)), dma, dma((2,)), dma, dma,
        ],
        compiler_params=pltpu.CompilerParams(collective_id=0, has_side_effects=True),
    )(right_side, links, coefs.reshape(1, count), reaction.reshape(1, count))
    return pl.pallas_call(
        write_out,
        out_shape=(
            jax.ShapeDtypeStruct((nrhs, count), jnp.float32),
            jax.ShapeDtypeStruct((SWEEPS, nrhs), jnp.float32),
        ),
        in_specs=[vmem, vmem],
        out_specs=[pl.BlockSpec(memory_space=pl.ANY)] * 2,
        scratch_shapes=[dma((2,))],
    )(*[pltpu.with_memory_space_constraint(f, pltpu.VMEM) for f in found])


def in_one_kernel(mesh):
    return mesh.shape["grp"] == SUB // CX and 2 * SUB <= mesh.shape["row"] <= 4 * SUB


def solution(mesh):
    body = on_device
    if in_one_kernel(mesh):
        body = functools.partial(whole_sweeps, mesh.shape["grp"], mesh.shape["row"])
    return jax.shard_map(
        body,
        mesh=mesh,
        in_specs=(
            P(None, ("grp", "row")),
            P(None, ("grp", "row")),
            P(("grp", "row")),
            P(("grp", "row")),
        ),
        out_specs=(P(None, ("grp", "row")), P()),
        check_vma=False,
    )
```

```python
import functools
import math

import jax
import jax.numpy as jnp
import numpy as np
from jax import lax
from jax.experimental import pallas as pl
from jax.experimental.pallas import tpu as pltpu
from jax.sharding import PartitionSpec as P

SWEEPS = 2
DEGREE = 4
CX, CY, CZ = 4, 2, 16
SUB, LANES = 8, 128
MESH = pl.DeviceIdType.MESH
HIGHEST = lax.Precision.HIGHEST


def shifted(block, axis, distance):
    devices = range(lax.axis_size(axis))
    route = [((i - distance) % len(devices), i) for i in devices]
    return lax.ppermute(block, axis, route)


def element_matrix():
    node_ids = np.arange(8)
    corner = np.stack([node_ids % 2, node_ids // 2 % 2, node_ids // 4], axis=1)
    gauss_points = np.array([0.5 - 0.5 / math.sqrt(3.0), 0.5 + 0.5 / math.sqrt(3.0)])
    stiffness = np.zeros((8, 8))
    for q in range(8):
        quad_point = gauss_points[np.array([q % 2, q // 2 % 2, q // 4])]
        values = np.where(corner > 0.5, quad_point, 1.0 - quad_point)
        slopes = np.where(corner > 0.5, 1.0, -1.0)
        gradient = np.stack(
            [
                slopes[:, 0] * values[:, 1] * values[:, 2],
                values[:, 0] * slopes[:, 1] * values[:, 2],
                values[:, 0] * values[:, 1] * slopes[:, 2],
            ],
            axis=1,
        )
        stiffness = stiffness + gradient @ gradient.T / 8.0
    return stiffness


def element_images(window, offsets, weights, stiffness):
    corners = window[:, offsets]
    images = (
        jnp.einsum("ml,rle->rme", stiffness, corners, precision=lax.Precision.HIGHEST) * weights
    )
    return jnp.zeros_like(window).at[:, offsets].add(images)


def on_device(right_side, links, coefs, reaction):
    stiffness = jnp.asarray(element_matrix(), dtype=jnp.float32)
    count = right_side.shape[1]
    groups = lax.axis_size("grp")
    rowcount = lax.axis_size("row")
    group_id = lax.axis_index("grp")
    row_id = lax.axis_index("row")
    total = count * groups * rowcount
    owner = links // count
    slot = links % count
    first = jnp.mod(owner // rowcount - group_id, groups)
    second = jnp.mod(owner % rowcount - row_id, rowcount)
    offsets = (first * 2 + second) * count + slot

    def apply_operator(field):
        above_row = shifted(field, "row", -1)
        upper = shifted(jnp.stack([field, above_row], axis=0), "grp", -1)
        window = jnp.concatenate([field, above_row, upper[0], upper[1]], axis=1)
        summed = element_images(window, offsets, coefs, stiffness)
        back = shifted(
            jnp.stack([summed[:, 2 * count : 3 * count], summed[:, 3 * count :]], axis=0), "grp", 1
        )
        first_col = summed[:, :count] + back[0]
        second_col = summed[:, count : 2 * count] + back[1]
        first_col = first_col + shifted(second_col, "row", 1)
        return first_col + reaction * field

    image = apply_operator(right_side)
    cross, square = lax.psum(
        (jnp.sum(right_side * image, axis=1), jnp.sum(image * image, axis=1)), ("grp", "row")
    )
    theta = square / cross
    upper = (1.5 * theta)[:, None]
    lower = upper / 10.0
    center = (upper + lower) / 2.0
    half = (upper - lower) / 2.0
    sigma = center / half
    solution = jnp.zeros_like(right_side)
    residual = right_side
    history = []
    for sweep in range(SWEEPS):
        start = residual
        correction = jnp.zeros_like(right_side)
        rho_now = 1.0 / sigma
        direction = residual / center
        for step in range(DEGREE):
            correction = correction + direction
            residual = residual - apply_operator(direction)
            if step + 1 < DEGREE:
                rho_next = 1.0 / (2.0 * sigma - rho_now)
                direction = rho_next * rho_now * direction + 2.0 * rho_next / half * residual
                rho_now = rho_next
        change = start - residual
        along, length, begin = lax.psum(
            (
                jnp.sum(start * change, axis=1),
                jnp.sum(change * change, axis=1),
                jnp.sum(start * start, axis=1),
            ),
            ("grp", "row"),
        )
        omega = along / length
        residual = start - omega[:, None] * change
        squares = begin - 2.0 * omega * along + omega * omega * length
        solution = solution + omega[:, None] * correction
        history.append(jnp.sqrt(squares / total))
    return (solution, jnp.stack(history, axis=0))


def thirds(a):
    high = a.astype(jnp.bfloat16).astype(jnp.float32)
    rest = a - high
    middle = rest.astype(jnp.bfloat16).astype(jnp.float32)
    return [high, middle, rest - middle]


def added(parts):
    high, middle, low = parts
    return high + middle + low


def turned(a, distance, axis=1):
    return pltpu.roll(a, distance % a.shape[axis], axis)


def tile_iota(axis):
    return lax.broadcasted_iota(jnp.int32, (SUB, LANES), axis)


def exchanged(tile):
    sub, low = tile_iota(0), tile_iota(1)
    for unit, radix in ((1, 4), (4, 2)):
        ahead = low // unit % radix - sub // unit % radix
        result = tile
        for k in range(1 - radix, radix):
            if k:
                moved = turned(turned(tile, -k * unit, 0), k * unit)
                result = jnp.where(ahead == k, moved, result)
        tile = result
    return tile


def paired(first, second):
    top = tile_iota(0) < SUB // 2
    return (
        jnp.where(top, first, turned(second, SUB // 2, 0)),
        jnp.where(top, turned(first, SUB // 2, 0), second),
    )


def correction_weights():
    center, half = (1.5 + 0.15) / 2.0, (1.5 - 0.15) / 2.0
    sigma = center / half
    rho_now = 1.0 / sigma
    direction, residual = np.zeros(DEGREE + 1), np.zeros(DEGREE + 1)
    correction = np.zeros(DEGREE + 1)
    residual[0], direction[0] = 1.0, 1.0 / center
    for _ in range(DEGREE):
        correction = correction + direction
        residual = residual - np.roll(direction, 1)
        rho_next = 1.0 / (2.0 * sigma - rho_now)
        direction = rho_next * rho_now * direction + 2.0 * rho_next / half * residual
        rho_now = rho_next
    return [float(b / correction[DEGREE - 1]) for b in correction[: DEGREE - 1]]


class Total:
    def __init__(self):
        self.parts = [None] * 4
        self.at = 0

    def add(self, value):
        k = self.at % 4
        self.parts[k] = value if self.parts[k] is None else self.parts[k] + value
        self.at += 1

    def folded(self):
        a, b, c, d = self.parts
        value = (a + b) + (c + d)
        for bit in (4, 2, 1):
            value = value + turned(value, bit, 0)
        return value


def over_z(value):
    parts = [value] + [turned(value, SUB * k) for k in range(1, LANES // SUB)]
    while len(parts) > 1:
        parts = [a + b for a, b in zip(parts[::2], parts[1::2])]
    return parts[0]


def summed(first, second):
    top = tile_iota(0) < SUB // 2
    both = over_z(jnp.where(top, first.folded(), second.folded()))
    other = turned(both, SUB // 2, 0)
    return jnp.where(top, both, other), jnp.where(top, other, both)


def kernel(
    groups, rowcount, total,
    right_hbm, links_hbm, coefs_hbm, react_hbm,
    solution_ref, rms_ref,
    right_ref, links_ref, coefs_ref, react_ref,
    auxout, auxin, outbox, inbox, answers, solved, order, spread, wide,
    masses, masses_z, flats, flats_z, talls, edges_x, edges_y, edges_z, edges_below, diag,
    bases, changes, corrections, powers, mixes,
    in_sem, out_send, aux_recv, out_recv, back_send, back_recv,
):
    nrhs, count = right_ref.shape
    leaders = nrhs // SUB
    near, second = leaders - CY, CY
    blocks = groups * rowcount
    planes = rowcount * CY
    grp = lax.axis_index("grp")
    row = lax.axis_index("row")
    me = grp * rowcount + row
    leading = row < jnp.where(grp == 0, near, second)
    rank = jnp.where(grp == 0, row, near + row)

    def leader(t):
        if isinstance(t, int):
            return (0, t) if t < near else (1, t - near)
        return (jnp.where(t < near, 0, 1), jnp.where(t < near, t, t - near))

    def block(b):
        return (b // rowcount, lax.rem(b, rowcount))

    def place_of(t):
        return jnp.where(t < near, t, rowcount + t - near)

    def another(k):
        return jnp.where(k < rank, k, k + 1)

    barrier = pltpu.get_barrier_semaphore()

    @pl.when(leading)
    def _():
        def nearness(place):
            d, o = place
            return abs(2 * o - rowcount) - rowcount // 2 * d - CX * (o % CX == CX // 2)

        peers = [(d, o) for d in range(groups) for o in range(rowcount) if d or o]
        for d, o in sorted(peers, key=nearness):
            peer = (lax.rem(grp + d, groups), lax.rem(row + o, rowcount))
            pl.semaphore_signal(barrier, inc=1, device_id=peer, device_id_type=MESH)

    loads = [
        pltpu.make_async_copy(source, target, in_sem)
        for source, target in (
            [(links_hbm, links_ref), (coefs_hbm, coefs_ref), (react_hbm, react_ref), (right_hbm, right_ref)]
        )
    ]
    for load in loads:
        load.start()

    lane = lax.broadcasted_iota(jnp.int32, (count, count), 1)
    down = lax.broadcasted_iota(jnp.int32, (count, count), 0)
    same_z = (down // SUB == lane // SUB).astype(jnp.float32)
    spread[0:count] = same_z
    spread[count : 2 * count] = same_z
    low = tile_iota(1)
    element = ((low % CX) * CY + low // CX % CY) * CZ + low // SUB

    def to_lanes(line):
        return jnp.take_along_axis(jnp.broadcast_to(line, (SUB, count)), element, axis=1)[0:1]

    everything = spread.at[pl.ds(0, links_ref.shape[0] + 2 + nrhs)]
    pltpu.make_async_copy(everything, everything, in_sem).wait()
    slots = to_lanes(links_ref[0:1, :] - me * count)
    order[...] = (down == slots).astype(jnp.float32)
    mass = to_lanes(coefs_ref[...] * (1.0 / 12.0))
    react = thirds(react_ref[...])
    react = jnp.concatenate(react + [jnp.zeros((SUB - 3, count), jnp.float32)], axis=0)
    stack = jnp.concatenate([react] + thirds(right_ref[...]), axis=0)
    stack = jnp.dot(stack, order[...], preferred_element_type=jnp.float32)
    react = added([stack[k : k + 1] for k in range(3)])
    auxout[...] = jnp.concatenate([mass, react], axis=0)
    field = added([stack[SUB + k * nrhs : SUB + (k + 1) * nrhs] for k in range(3)])

    own_part = jnp.where(row < rowcount // 2, 0, 1)

    def post(t, source, target, send, recv):
        return pltpu.make_async_remote_copy(
            src_ref=source(t), dst_ref=target.at[me], send_sem=send, recv_sem=recv,
            device_id=leader(t), device_id_type=MESH,
        )

    def post_aux(t):
        return post(t, lambda t: auxout, auxin, out_send, aux_recv.at[own_part])

    def post_field(t):
        return post(t, lambda t: outbox.at[t], inbox, out_send, out_recv.at[own_part])

    def start_posts():
        for send in (post_aux, post_field):

            @pl.when(leading)
            def _(send=send):
                for k in range(leaders - 1):
                    send(another(k)).start()

            @pl.when(jnp.logical_not(leading))
            def _(send=send):
                for t in [*range(near - CY, near), *range(near - CY), *range(near, leaders)]:
                    send(t).start()

    def whole_of(ref, number, send, recv):
        return pltpu.make_async_remote_copy(
            src_ref=ref.at[pl.ds(0, number)], dst_ref=ref.at[pl.ds(0, number)],
            send_sem=send, recv_sem=recv, device_id=leader(0), device_id_type=MESH,
        )

    def sent_posts(number):
        whole_of(spread, number * (SUB + 2), out_send, out_recv.at[0]).wait_send()

    for t in range(leaders):
        outbox[t] = exchanged(field[t * SUB : (t + 1) * SUB])
    pl.semaphore_wait(barrier, jnp.where(leading, leaders - 1, leaders))

    start_posts()

    def reply(b):
        return pltpu.make_async_remote_copy(
            src_ref=solved.at[b], dst_ref=answers.at[rank],
            send_sem=back_send, recv_sem=back_recv,
            device_id=block(b), device_id_type=MESH,
        )

    leader_blocks = [g * rowcount + r for g, r in map(leader, range(leaders))]
    outside = [
        (g, r) for r in range(rowcount) for g in range(groups) if r >= (near, second)[g]
    ]

    @pl.when(leading)
    def _():
        own = tile_iota(1) % SUB == tile_iota(0)
        half = rowcount // 2

        def expand(part):
            rows = [(k, p * rowcount + part * half) for k in range(2) for p in range(groups)]
            for at, (k, begin) in enumerate(rows):
                high, middle, _ = thirds(auxin[begin : begin + half, k, :])
                wide[0, at * half : (at + 1) * half] = high
                wide[1, at * half : (at + 1) * half] = middle
            pieces = [
                jnp.concatenate(
                    [
                        jnp.where(own, wide[which, k : k + 1, :], 0.0)
                        for k in range(len(rows) * half)
                    ],
                    axis=0,
                )
                for which in range(2)
            ]
            tiles = jnp.dot(
                jnp.concatenate(pieces, axis=1), spread[...], preferred_element_type=jnp.float32
            )
            tiles = [tiles[k * SUB : (k + 1) * SUB] for k in range(len(rows) * half)]
            for q in range(half):
                for k, m in enumerate(paired(tiles[q], tiles[half + q])):
                    y = CY * (part * half + q) + k
                    m_z = turned(m, SUB)
                    flat, flat_z = m + turned(m, 1, 0), m_z + turned(m_z, 1, 0)
                    masses[y], masses_z[y] = m, m_z
                    flats[y], flats_z[y] = flat, flat_z
                    talls[y], edges_y[y] = m + m_z, flat + flat_z
                for k, react in enumerate(paired(tiles[2 * half + q], tiles[3 * half + q])):
                    diag[CY * (part * half + q) + k] = react

        def settle(ys):
            for y in ys:
                z = (y - 1) % planes
                edges_x[y] = talls[y] + talls[z]
                edges_z[y] = flats[y] + flats[z]
                edges_below[y] = flats_z[y] + flats_z[z]
                diag[y] = diag[y] + 5.0 * (edges_y[y] + edges_y[z])

        def take_in(part):
            for q in range(part * half, (part + 1) * half):
                for k, value in enumerate(paired(inbox[q], inbox[rowcount + q])):
                    bases[0, CY * q + k] = value

        def apply_operator(source, sink, ys):
            taken, pushed = {}, {}

            def around(y):
                y = y % planes
                if y not in taken:
                    v = source(y)
                    above, below = turned(v, -SUB), turned(v, SUB)
                    up, down = v + above, v + below
                    up, down = up + turned(up, -1, 0), down + turned(down, -1, 0)
                    taken[y] = (v, above, below, up, down)
                return taken[y]

            def push(y):
                y = y % planes
                if y not in pushed:
                    (_, _, _, up, down), (_, _, _, next_up, next_down) = around(y), around(y + 1)
                    pushed[y] = masses[y] * (up + next_up) + masses_z[y] * (down + next_down)
                return pushed[y]

            for y in ys:
                v, above, below, _, _ = around(y)
                both = push(y) + push(y - 1)
                edge_x = edges_x[y]
                image = (diag[y] * v + edges_z[y] * above) + edges_below[y] * below
                image = image + (
                    edges_y[y] * around(y + 1)[0] + edges_y[(y - 1) % planes] * around(y - 1)[0]
                )
                image = image + (edge_x * turned(v, -1, 0) - both)
                sink(y, image + turned(edge_x * v - both, 1, 0))

        square, cross = Total(), Total()

        def opening_image(y, image):
            powers[0, y] = image
            square.add(image * image)
            cross.add(bases[0, y] * image)

        def stored(sweep, k):
            def sink(y, image):
                powers[sweep * DEGREE + k, y] = image

            return sink

        def mixed(factors, terms):
            value = factors[0] * terms[0]
            for factor, term in zip(factors[1:], terms[1:]):
                value = value + factor * term
            return value

        def ring(begin):
            return [(begin + k) % planes for k in range(planes)]

        def early(k):
            return range(k, planes // 2 - k)

        def late(k):
            return [y for y in ring(planes // 2 - k) if y not in early(k)]

        def start_plane(y):
            return bases[0, y]

        def first_image(y):
            return powers[0, y]

        auxin[me] = auxout[...]
        inbox[me] = outbox[rank]
        for part, ys in ((0, range(1, planes // 2)), (1, ring(planes // 2)[: planes // 2 + 1])):
            number = blocks // 2 - 1 + part
            whole_of(auxin, number, out_send, aux_recv.at[part]).wait_recv()
            expand(part)
            settle(ys)
            whole_of(inbox, number, out_send, out_recv.at[part]).wait_recv()
            take_in(part)
            if part == 0:
                apply_operator(start_plane, opening_image, early(1))
                apply_operator(first_image, stored(0, 1), early(2))
                apply_operator(lambda y: powers[1, y], stored(0, 2), early(3))
        apply_operator(start_plane, opening_image, late(1))
        square, cross = summed(square, cross)
        theta = square / cross
        scales = [theta]
        for _ in range(DEGREE - 2):
            scales.append(scales[-1] * theta)
        factors = [b * scale for b, scale in zip(correction_weights(), scales[::-1])]

        def corrected(sweep):
            def source(y):
                begin = sweep * DEGREE
                terms = [bases[sweep, y]] + [powers[begin + k, y] for k in range(DEGREE - 2)]
                value = powers[begin + DEGREE - 2, y] + mixed(factors, terms)
                corrections[sweep, y] = value
                return value

            return source

        def finishing(sweep, along, length):
            def sink(y, change):
                along.add(bases[sweep, y] * change)
                length.add(change * change)
                changes[y] = change

            return sink

        along, length = Total(), Total()
        apply_operator(first_image, stored(0, 1), late(2))
        apply_operator(lambda y: powers[1, y], stored(0, 2), late(3))
        begin_at = planes // 2 - DEGREE + 1
        apply_operator(corrected(0), finishing(0, along, length), ring(begin_at))
        apply_operator(lambda y: changes[y], stored(0, 3), ring(begin_at + 1))
        along, length = summed(along, length)
        omega = along / length
        begin = Total()

        def second_start(y):
            base = bases[0, y] - omega * changes[y]
            bases[1, y] = base
            begin.add(base * base)
            image = powers[0, y] - omega * powers[3, y]
            powers[DEGREE, y] = image
            return image

        apply_operator(second_start, stored(1, 1), ring(begin_at + 2))
        began = over_z(begin.folded())
        apply_operator(lambda y: powers[DEGREE + 1, y], stored(1, 2), ring(begin_at + 3))
        along, length = Total(), Total()
        apply_operator(corrected(1), finishing(1, along, length), ring(begin_at + 4))
        for q in range(rowcount):
            for sweep in range(SWEEPS):
                halves = [corrections[sweep, CY * q + k] for k in range(CY)]
                if sweep == 0:
                    halves = [omega * value for value in halves]
                for p, tile in enumerate(paired(*halves)):
                    mixes[sweep, p * rowcount + q] = tile
        along, length = summed(along, length)
        omega = along / length
        group = tile_iota(1) // SUB
        last = jnp.maximum(began - omega * along, 0.0)
        rms = jnp.where(group == rank, began, jnp.where(group == rank + leaders, last, 0.0))
        rms = jnp.sqrt(rms / total)[0:1]

        def settled(b):
            solved[b, 0:SUB] = mixes[0, b] + omega * mixes[1, b]
            solved[b, SUB : SUB + 1] = rms

        for group in (leader_blocks[:CY], leader_blocks[CY:]):
            for b in group:
                settled(b)
            for b in group:

                @pl.when(me != b)
                def _(b=b):
                    reply(b).start()

        for b in [g * rowcount + r for g, r in sorted(outside, key=lambda p: (p[1] % CX, p[1]))]:
            settled(b)
            reply(b).start()
        answers[rank] = solved[me]

    def answered(number):
        whole_of(answers, number, back_send, back_recv).wait_recv()

    @pl.when(leading)
    def _():
        answered(leaders - 1)

    @pl.when(jnp.logical_not(leading))
    def _():
        answered(leaders)

    whole = jnp.concatenate([exchanged(answers[t, 0:SUB]) for t in range(leaders)], axis=0)
    whole = jnp.concatenate(thirds(whole), axis=0)
    whole = lax.dot_general(
        whole, order[...], (((1,), (1,)), ((), ())), preferred_element_type=jnp.float32
    )
    solution_ref[...] = added([whole[k * nrhs : (k + 1) * nrhs] for k in range(3)])
    line = answers[0, SUB : SUB + 1]
    for t in range(1, leaders):
        line = line + answers[t, SUB : SUB + 1]
    other = turned(line, count // 2)
    rms_ref[...] = jnp.concatenate([line, other], axis=0)[:, :nrhs]

    @pl.when(leading)
    def _():
        sent_posts(leaders - 1)
        whole_of(solved, blocks - 1, back_send, back_recv).wait_send()

    @pl.when(jnp.logical_not(leading))
    def _():
        sent_posts(leaders)


def write_out(solution_ref, rms_ref, out_hbm, rms_hbm, sems):
    copies = [
        pltpu.make_async_copy(solution_ref, out_hbm, sems.at[0]),
        pltpu.make_async_copy(rms_ref, rms_hbm, sems.at[1]),
    ]
    for copy in copies:
        copy.start()
    for copy in copies:
        copy.wait()


def whole_sweeps(groups, rowcount, right_side, links, coefs, reaction):
    nrhs, count = right_side.shape
    leaders = nrhs // SUB
    blocks = groups * rowcount
    planes = rowcount * CY
    dma = pltpu.SemaphoreType.DMA
    vmem = pl.BlockSpec(memory_space=pltpu.VMEM)

    def space(*shape):
        return pltpu.VMEM(shape, jnp.float32)

    plane = space(planes, SUB, count)
    twice = space(SWEEPS, planes, SUB, count)
    found = pl.pallas_call(
        functools.partial(kernel, groups, rowcount, count * groups * rowcount),
        out_shape=(pltpu.VMEM((nrhs, count), jnp.float32), pltpu.VMEM((SWEEPS, nrhs), jnp.float32)),
        in_specs=[pl.BlockSpec(memory_space=pl.ANY)] * 4,
        out_specs=(vmem, vmem),
        scratch_shapes=[
            space(nrhs, count), pltpu.VMEM(links.shape, jnp.int32), space(1, count), space(1, count),
            space(2, count), space(blocks, 2, count),
            space(leaders, SUB, count), space(blocks, SUB, count),
            space(leaders, SUB + 1, count), space(blocks, SUB + 1, count),
            space(count, count), space(2 * count, count), space(2, 2 * blocks, count),
            plane, plane, plane, plane, plane, plane, plane, plane, plane, plane,
            twice, plane, twice, space(SWEEPS * DEGREE, planes, SUB, count),
            space(SWEEPS, blocks, SUB, count),
            dma, dma, dma((2,)), dma((2,)), dma, dma,
        ],
        compiler_params=pltpu.CompilerParams(collective_id=0, has_side_effects=True),
    )(right_side, links, coefs.reshape(1, count), reaction.reshape(1, count))
    return pl.pallas_call(
        write_out,
        out_shape=(
            jax.ShapeDtypeStruct((nrhs, count), jnp.float32),
            jax.ShapeDtypeStruct((SWEEPS, nrhs), jnp.float32),
        ),
        in_specs=[vmem, vmem],
        out_specs=[pl.BlockSpec(memory_space=pl.ANY)] * 2,
        scratch_shapes=[dma((2,))],
    )(*[pltpu.with_memory_space_constraint(f, pltpu.VMEM) for f in found])


def in_one_kernel(mesh):
    return mesh.shape["grp"] == SUB // CX and 2 * SUB <= mesh.shape["row"] <= 4 * SUB


def solution(mesh):
    body = on_device
    if in_one_kernel(mesh):
        body = functools.partial(whole_sweeps, mesh.shape["grp"], mesh.shape["row"])
    return jax.shard_map(
        body,
        mesh=mesh,
        in_specs=(
            P(None, ("grp", "row")),
            P(None, ("grp", "row")),
            P(("grp", "row")),
            P(("grp", "row")),
        ),
        out_specs=(P(None, ("grp", "row")), P()),
        check_vma=False,
    )
```

```python
import functools
import math

import jax
import jax.numpy as jnp
import numpy as np
from jax import lax
from jax.experimental import pallas as pl
from jax.experimental.pallas import tpu as pltpu
from jax.sharding import PartitionSpec as P

SWEEPS = 2
DEGREE = 4
CX, CY, CZ = 4, 2, 16
SUB, LANES = 8, 128
MESH = pl.DeviceIdType.MESH
HIGHEST = lax.Precision.HIGHEST


def shifted(block, axis, distance):
    devices = range(lax.axis_size(axis))
    route = [((i - distance) % len(devices), i) for i in devices]
    return lax.ppermute(block, axis, route)


def element_matrix():
    node_ids = np.arange(8)
    corner = np.stack([node_ids % 2, node_ids // 2 % 2, node_ids // 4], axis=1)
    gauss_points = np.array([0.5 - 0.5 / math.sqrt(3.0), 0.5 + 0.5 / math.sqrt(3.0)])
    stiffness = np.zeros((8, 8))
    for q in range(8):
        quad_point = gauss_points[np.array([q % 2, q // 2 % 2, q // 4])]
        values = np.where(corner > 0.5, quad_point, 1.0 - quad_point)
        slopes = np.where(corner > 0.5, 1.0, -1.0)
        gradient = np.stack(
            [
                slopes[:, 0] * values[:, 1] * values[:, 2],
                values[:, 0] * slopes[:, 1] * values[:, 2],
                values[:, 0] * values[:, 1] * slopes[:, 2],
            ],
            axis=1,
        )
        stiffness = stiffness + gradient @ gradient.T / 8.0
    return stiffness


def element_images(window, offsets, weights, stiffness):
    corners = window[:, offsets]
    images = (
        jnp.einsum("ml,rle->rme", stiffness, corners, precision=lax.Precision.HIGHEST) * weights
    )
    return jnp.zeros_like(window).at[:, offsets].add(images)


def on_device(right_side, links, coefs, reaction):
    stiffness = jnp.asarray(element_matrix(), dtype=jnp.float32)
    count = right_side.shape[1]
    groups = lax.axis_size("grp")
    rowcount = lax.axis_size("row")
    group_id = lax.axis_index("grp")
    row_id = lax.axis_index("row")
    total = count * groups * rowcount
    owner = links // count
    slot = links % count
    first = jnp.mod(owner // rowcount - group_id, groups)
    second = jnp.mod(owner % rowcount - row_id, rowcount)
    offsets = (first * 2 + second) * count + slot

    def apply_operator(field):
        above_row = shifted(field, "row", -1)
        upper = shifted(jnp.stack([field, above_row], axis=0), "grp", -1)
        window = jnp.concatenate([field, above_row, upper[0], upper[1]], axis=1)
        summed = element_images(window, offsets, coefs, stiffness)
        back = shifted(
            jnp.stack([summed[:, 2 * count : 3 * count], summed[:, 3 * count :]], axis=0), "grp", 1
        )
        first_col = summed[:, :count] + back[0]
        second_col = summed[:, count : 2 * count] + back[1]
        first_col = first_col + shifted(second_col, "row", 1)
        return first_col + reaction * field

    image = apply_operator(right_side)
    cross, square = lax.psum(
        (jnp.sum(right_side * image, axis=1), jnp.sum(image * image, axis=1)), ("grp", "row")
    )
    theta = square / cross
    upper = (1.5 * theta)[:, None]
    lower = upper / 10.0
    center = (upper + lower) / 2.0
    half = (upper - lower) / 2.0
    sigma = center / half
    solution = jnp.zeros_like(right_side)
    residual = right_side
    history = []
    for sweep in range(SWEEPS):
        start = residual
        correction = jnp.zeros_like(right_side)
        rho_now = 1.0 / sigma
        direction = residual / center
        for step in range(DEGREE):
            correction = correction + direction
            residual = residual - apply_operator(direction)
            if step + 1 < DEGREE:
                rho_next = 1.0 / (2.0 * sigma - rho_now)
                direction = rho_next * rho_now * direction + 2.0 * rho_next / half * residual
                rho_now = rho_next
        change = start - residual
        along, length, begin = lax.psum(
            (
                jnp.sum(start * change, axis=1),
                jnp.sum(change * change, axis=1),
                jnp.sum(start * start, axis=1),
            ),
            ("grp", "row"),
        )
        omega = along / length
        residual = start - omega[:, None] * change
        squares = begin - 2.0 * omega * along + omega * omega * length
        solution = solution + omega[:, None] * correction
        history.append(jnp.sqrt(squares / total))
    return (solution, jnp.stack(history, axis=0))


def thirds(a):
    high = a.astype(jnp.bfloat16).astype(jnp.float32)
    rest = a - high
    middle = rest.astype(jnp.bfloat16).astype(jnp.float32)
    return [high, middle, rest - middle]


def added(parts):
    high, middle, low = parts
    return high + middle + low


def turned(a, distance, axis=1):
    return pltpu.roll(a, distance % a.shape[axis], axis)


def tile_iota(axis):
    return lax.broadcasted_iota(jnp.int32, (SUB, LANES), axis)


def exchanged(tile):
    sub, low = tile_iota(0), tile_iota(1)
    for unit, radix in ((1, 4), (4, 2)):
        ahead = low // unit % radix - sub // unit % radix
        result = tile
        for k in range(1 - radix, radix):
            if k:
                moved = turned(turned(tile, -k * unit, 0), k * unit)
                result = jnp.where(ahead == k, moved, result)
        tile = result
    return tile


def paired(first, second):
    top = tile_iota(0) < SUB // 2
    return (
        jnp.where(top, first, turned(second, SUB // 2, 0)),
        jnp.where(top, turned(first, SUB // 2, 0), second),
    )


def correction_weights():
    center, half = (1.5 + 0.15) / 2.0, (1.5 - 0.15) / 2.0
    sigma = center / half
    rho_now = 1.0 / sigma
    direction, residual = np.zeros(DEGREE + 1), np.zeros(DEGREE + 1)
    correction = np.zeros(DEGREE + 1)
    residual[0], direction[0] = 1.0, 1.0 / center
    for _ in range(DEGREE):
        correction = correction + direction
        residual = residual - np.roll(direction, 1)
        rho_next = 1.0 / (2.0 * sigma - rho_now)
        direction = rho_next * rho_now * direction + 2.0 * rho_next / half * residual
        rho_now = rho_next
    return [float(b / correction[DEGREE - 1]) for b in correction[: DEGREE - 1]]


class Total:
    def __init__(self):
        self.parts = [None] * 4
        self.at = 0

    def add(self, value):
        k = self.at % 4
        self.parts[k] = value if self.parts[k] is None else self.parts[k] + value
        self.at += 1

    def folded(self):
        a, b, c, d = self.parts
        value = (a + b) + (c + d)
        for bit in (4, 2, 1):
            value = value + turned(value, bit, 0)
        return value


def over_z(value):
    parts = [value] + [turned(value, SUB * k) for k in range(1, LANES // SUB)]
    while len(parts) > 1:
        parts = [a + b for a, b in zip(parts[::2], parts[1::2])]
    return parts[0]


def summed(first, second):
    top = tile_iota(0) < SUB // 2
    both = over_z(jnp.where(top, first.folded(), second.folded()))
    other = turned(both, SUB // 2, 0)
    return jnp.where(top, both, other), jnp.where(top, other, both)


def kernel(
    groups, rowcount, total,
    right_hbm, links_hbm, coefs_hbm, react_hbm,
    solution_ref, rms_ref,
    right_ref, links_ref, coefs_ref, react_ref,
    auxout, auxin, outbox, inbox, answers, solved, order, spread, wide,
    masses, masses_z, flats, flats_z, talls, edges_x, edges_y, edges_z, edges_below, diag,
    bases, changes, corrections, powers, mixes,
    in_sem, out_send, aux_recv, out_recv, back_send, back_recv,
):
    nrhs, count = right_ref.shape
    leaders = nrhs // SUB
    near, second = leaders - CY, CY
    blocks = groups * rowcount
    planes = rowcount * CY
    grp = lax.axis_index("grp")
    row = lax.axis_index("row")
    me = grp * rowcount + row
    leading = row < jnp.where(grp == 0, near, second)
    rank = jnp.where(grp == 0, row, near + row)

    def leader(t):
        if isinstance(t, int):
            return (0, t) if t < near else (1, t - near)
        return (jnp.where(t < near, 0, 1), jnp.where(t < near, t, t - near))

    def block(b):
        return (b // rowcount, lax.rem(b, rowcount))

    def place_of(t):
        return jnp.where(t < near, t, rowcount + t - near)

    def another(k):
        return jnp.where(k < rank, k, k + 1)

    barrier = pltpu.get_barrier_semaphore()

    @pl.when(leading)
    def _():
        def nearness(place):
            d, o = place
            return abs(2 * o - rowcount) - rowcount // 2 * d - CX * (o % CX == CX // 2)

        peers = [(d, o) for d in range(groups) for o in range(rowcount) if d or o]
        for d, o in sorted(peers, key=nearness):
            peer = (lax.rem(grp + d, groups), lax.rem(row + o, rowcount))
            pl.semaphore_signal(barrier, inc=1, device_id=peer, device_id_type=MESH)

    loads = [
        pltpu.make_async_copy(source, target, in_sem)
        for source, target in (
            [(links_hbm, links_ref), (coefs_hbm, coefs_ref), (react_hbm, react_ref), (right_hbm, right_ref)]
        )
    ]
    for load in loads:
        load.start()

    lane = lax.broadcasted_iota(jnp.int32, (count, count), 1)
    down = lax.broadcasted_iota(jnp.int32, (count, count), 0)
    same_z = (down // SUB == lane // SUB).astype(jnp.float32)
    spread[0:count] = same_z
    spread[count : 2 * count] = same_z
    low = tile_iota(1)
    element = ((low % CX) * CY + low // CX % CY) * CZ + low // SUB

    def to_lanes(line):
        return jnp.take_along_axis(jnp.broadcast_to(line, (SUB, count)), element, axis=1)[0:1]

    everything = spread.at[pl.ds(0, links_ref.shape[0] + 2 + nrhs)]
    pltpu.make_async_copy(everything, everything, in_sem).wait()
    slots = to_lanes(links_ref[0:1, :] - me * count)
    order[...] = (down == slots).astype(jnp.float32)
    mass = to_lanes(coefs_ref[...] * (1.0 / 12.0))
    react = thirds(react_ref[...])
    react = jnp.concatenate(react + [jnp.zeros((SUB - 3, count), jnp.float32)], axis=0)
    stack = jnp.concatenate([react] + thirds(right_ref[...]), axis=0)
    stack = jnp.dot(stack, order[...], preferred_element_type=jnp.float32)
    react = added([stack[k : k + 1] for k in range(3)])
    auxout[...] = jnp.concatenate([mass, react], axis=0)
    field = added([stack[SUB + k * nrhs : SUB + (k + 1) * nrhs] for k in range(3)])

    own_part = jnp.where(row < rowcount // 2, 0, 1)

    def post(t, source, target, send, recv):
        return pltpu.make_async_remote_copy(
            src_ref=source(t), dst_ref=target.at[me], send_sem=send, recv_sem=recv,
            device_id=leader(t), device_id_type=MESH,
        )

    def post_aux(t):
        return post(t, lambda t: auxout, auxin, out_send, aux_recv.at[own_part])

    def post_field(t):
        return post(t, lambda t: outbox.at[t], inbox, out_send, out_recv.at[own_part])

    def start_posts():
        for send in (post_aux, post_field):

            @pl.when(leading)
            def _(send=send):
                for k in range(leaders - 1):
                    send(another(k)).start()

            @pl.when(jnp.logical_not(leading))
            def _(send=send):
                for t in [*range(near - CY, near), *range(near - CY), *range(near, leaders)]:
                    send(t).start()

    def whole_of(ref, number, send, recv):
        return pltpu.make_async_remote_copy(
            src_ref=ref.at[pl.ds(0, number)], dst_ref=ref.at[pl.ds(0, number)],
            send_sem=send, recv_sem=recv, device_id=leader(0), device_id_type=MESH,
        )

    def sent_posts(number):
        whole_of(spread, number * (SUB + 2), out_send, out_recv.at[0]).wait_send()

    for t in range(leaders):
        outbox[t] = exchanged(field[t * SUB : (t + 1) * SUB])
    pl.semaphore_wait(barrier, jnp.where(leading, leaders - 1, leaders))

    start_posts()

    def reply(b):
        return pltpu.make_async_remote_copy(
            src_ref=solved.at[b], dst_ref=answers.at[rank],
            send_sem=back_send, recv_sem=back_recv,
            device_id=block(b), device_id_type=MESH,
        )

    leader_blocks = [g * rowcount + r for g, r in map(leader, range(leaders))]
    outside = [
        (g, r) for r in range(rowcount) for g in range(groups) if r >= (near, second)[g]
    ]

    @pl.when(leading)
    def _():
        own = tile_iota(1) % SUB == tile_iota(0)
        half = rowcount // 2

        def expand(part):
            rows = [(k, p * rowcount + part * half) for k in range(2) for p in range(groups)]
            for at, (k, begin) in enumerate(rows):
                high, middle, _ = thirds(auxin[begin : begin + half, k, :])
                wide[0, at * half : (at + 1) * half] = high
                wide[1, at * half : (at + 1) * half] = middle
            pieces = [
                jnp.concatenate(
                    [
                        jnp.where(own, wide[which, k : k + 1, :], 0.0)
                        for k in range(len(rows) * half)
                    ],
                    axis=0,
                )
                for which in range(2)
            ]
            tiles = jnp.dot(
                jnp.concatenate(pieces, axis=1), spread[...], preferred_element_type=jnp.float32
            )
            tiles = [tiles[k * SUB : (k + 1) * SUB] for k in range(len(rows) * half)]
            for q in range(half):
                for k, m in enumerate(paired(tiles[q], tiles[half + q])):
                    y = CY * (part * half + q) + k
                    m_z = turned(m, SUB)
                    flat, flat_z = m + turned(m, 1, 0), m_z + turned(m_z, 1, 0)
                    masses[y], masses_z[y] = m, m_z
                    flats[y], flats_z[y] = flat, flat_z
                    talls[y], edges_y[y] = m + m_z, flat + flat_z
                for k, react in enumerate(paired(tiles[2 * half + q], tiles[3 * half + q])):
                    diag[CY * (part * half + q) + k] = react

        def settle(ys):
            for y in ys:
                z = (y - 1) % planes
                edges_x[y] = talls[y] + talls[z]
                edges_z[y] = flats[y] + flats[z]
                edges_below[y] = flats_z[y] + flats_z[z]
                diag[y] = diag[y] + 5.0 * (edges_y[y] + edges_y[z])

        def take_in(part):
            for q in range(part * half, (part + 1) * half):
                for k, value in enumerate(paired(inbox[q], inbox[rowcount + q])):
                    bases[0, CY * q + k] = value

        def apply_operator(source, sink, ys):
            taken, pushed = {}, {}

            def around(y):
                y = y % planes
                if y not in taken:
                    v = source(y)
                    above, below = turned(v, -SUB), turned(v, SUB)
                    up, down = v + above, v + below
                    up, down = up + turned(up, -1, 0), down + turned(down, -1, 0)
                    taken[y] = (v, above, below, up, down)
                return taken[y]

            def push(y):
                y = y % planes
                if y not in pushed:
                    (_, _, _, up, down), (_, _, _, next_up, next_down) = around(y), around(y + 1)
                    pushed[y] = masses[y] * (up + next_up) + masses_z[y] * (down + next_down)
                return pushed[y]

            for y in ys:
                v, above, below, _, _ = around(y)
                both = push(y) + push(y - 1)
                edge_x = edges_x[y]
                image = (diag[y] * v + edges_z[y] * above) + edges_below[y] * below
                image = image + (
                    edges_y[y] * around(y + 1)[0] + edges_y[(y - 1) % planes] * around(y - 1)[0]
                )
                image = image + (edge_x * turned(v, -1, 0) - both)
                sink(y, image + turned(edge_x * v - both, 1, 0))

        square, cross = Total(), Total()

        def opening_image(y, image):
            powers[0, y] = image
            square.add(image * image)
            cross.add(bases[0, y] * image)

        def stored(sweep, k):
            def sink(y, image):
                powers[sweep * DEGREE + k, y] = image

            return sink

        def mixed(factors, terms):
            value = factors[0] * terms[0]
            for factor, term in zip(factors[1:], terms[1:]):
                value = value + factor * term
            return value

        def ring(begin):
            return [(begin + k) % planes for k in range(planes)]

        def early(k):
            return range(k, planes // 2 - k)

        def late(k):
            return [y for y in ring(planes // 2 - k) if y not in early(k)]

        def start_plane(y):
            return bases[0, y]

        def first_image(y):
            return powers[0, y]

        auxin[me] = auxout[...]
        inbox[me] = outbox[rank]
        for part, ys in ((0, range(1, planes // 2)), (1, ring(planes // 2)[: planes // 2 + 1])):
            number = blocks // 2 - 1 + part
            whole_of(auxin, number, out_send, aux_recv.at[part]).wait_recv()
            expand(part)
            settle(ys)
            whole_of(inbox, number, out_send, out_recv.at[part]).wait_recv()
            take_in(part)
            if part == 0:
                apply_operator(start_plane, opening_image, early(1))
                apply_operator(first_image, stored(0, 1), early(2))
                apply_operator(lambda y: powers[1, y], stored(0, 2), early(3))
        apply_operator(start_plane, opening_image, late(1))
        square, cross = summed(square, cross)
        theta = square / cross
        scales = [theta]
        for _ in range(DEGREE - 2):
            scales.append(scales[-1] * theta)
        factors = [b * scale for b, scale in zip(correction_weights(), scales[::-1])]

        def corrected(sweep):
            def source(y):
                begin = sweep * DEGREE
                terms = [bases[sweep, y]] + [powers[begin + k, y] for k in range(DEGREE - 2)]
                value = powers[begin + DEGREE - 2, y] + mixed(factors, terms)
                corrections[sweep, y] = value
                return value

            return source

        def finishing(sweep, along, length):
            def sink(y, change):
                along.add(bases[sweep, y] * change)
                length.add(change * change)
                changes[y] = change

            return sink

        along, length = Total(), Total()
        apply_operator(first_image, stored(0, 1), late(2))
        apply_operator(lambda y: powers[1, y], stored(0, 2), late(3))
        begin_at = planes // 2 - DEGREE + 1
        apply_operator(corrected(0), finishing(0, along, length), ring(begin_at))
        apply_operator(lambda y: changes[y], stored(0, 3), ring(begin_at + 1))
        along, length = summed(along, length)
        omega = along / length
        begin = Total()

        def second_start(y):
            base = bases[0, y] - omega * changes[y]
            bases[1, y] = base
            begin.add(base * base)
            image = powers[0, y] - omega * powers[3, y]
            powers[DEGREE, y] = image
            return image

        apply_operator(second_start, stored(1, 1), ring(begin_at + 2))
        began = over_z(begin.folded())
        apply_operator(lambda y: powers[DEGREE + 1, y], stored(1, 2), ring(begin_at + 3))
        along, length = Total(), Total()
        apply_operator(corrected(1), finishing(1, along, length), ring(begin_at + 4))
        for q in range(rowcount):
            for sweep in range(SWEEPS):
                halves = [corrections[sweep, CY * q + k] for k in range(CY)]
                if sweep == 0:
                    halves = [omega * value for value in halves]
                for p, tile in enumerate(paired(*halves)):
                    mixes[sweep, p * rowcount + q] = tile
        along, length = summed(along, length)
        omega = along / length
        group = tile_iota(1) // SUB
        last = jnp.maximum(began - omega * along, 0.0)
        rms = jnp.where(group == rank, began, jnp.where(group == rank + leaders, last, 0.0))
        rms = jnp.sqrt(rms / total)[0:1]

        def settled(b):
            solved[b, 0:SUB] = mixes[0, b] + omega * mixes[1, b]
            solved[b, SUB : SUB + 1] = rms

        for group in (leader_blocks[:CY], leader_blocks[CY:]):
            for b in group:
                settled(b)
            for b in group:

                @pl.when(me != b)
                def _(b=b):
                    reply(b).start()

        for b in [g * rowcount + r for g, r in sorted(outside, key=lambda p: -(p[0] + p[1] % CX // 2 + min(p[1] // CX, rowcount // CX - p[1] // CX)))]:
            settled(b)
            reply(b).start()
        answers[rank] = solved[me]

    def answered(number):
        whole_of(answers, number, back_send, back_recv).wait_recv()

    @pl.when(leading)
    def _():
        answered(leaders - 1)

    @pl.when(jnp.logical_not(leading))
    def _():
        answered(leaders)

    whole = jnp.concatenate([exchanged(answers[t, 0:SUB]) for t in range(leaders)], axis=0)
    whole = jnp.concatenate(thirds(whole), axis=0)
    whole = lax.dot_general(
        whole, order[...], (((1,), (1,)), ((), ())), preferred_element_type=jnp.float32
    )
    solution_ref[...] = added([whole[k * nrhs : (k + 1) * nrhs] for k in range(3)])
    line = answers[0, SUB : SUB + 1]
    for t in range(1, leaders):
        line = line + answers[t, SUB : SUB + 1]
    other = turned(line, count // 2)
    rms_ref[...] = jnp.concatenate([line, other], axis=0)[:, :nrhs]

    @pl.when(leading)
    def _():
        sent_posts(leaders - 1)
        whole_of(solved, blocks - 1, back_send, back_recv).wait_send()

    @pl.when(jnp.logical_not(leading))
    def _():
        sent_posts(leaders)


def write_out(solution_ref, rms_ref, out_hbm, rms_hbm, sems):
    copies = [
        pltpu.make_async_copy(solution_ref, out_hbm, sems.at[0]),
        pltpu.make_async_copy(rms_ref, rms_hbm, sems.at[1]),
    ]
    for copy in copies:
        copy.start()
    for copy in copies:
        copy.wait()


def whole_sweeps(groups, rowcount, right_side, links, coefs, reaction):
    nrhs, count = right_side.shape
    leaders = nrhs // SUB
    blocks = groups * rowcount
    planes = rowcount * CY
    dma = pltpu.SemaphoreType.DMA
    vmem = pl.BlockSpec(memory_space=pltpu.VMEM)

    def space(*shape):
        return pltpu.VMEM(shape, jnp.float32)

    plane = space(planes, SUB, count)
    twice = space(SWEEPS, planes, SUB, count)
    found = pl.pallas_call(
        functools.partial(kernel, groups, rowcount, count * groups * rowcount),
        out_shape=(pltpu.VMEM((nrhs, count), jnp.float32), pltpu.VMEM((SWEEPS, nrhs), jnp.float32)),
        in_specs=[pl.BlockSpec(memory_space=pl.ANY)] * 4,
        out_specs=(vmem, vmem),
        scratch_shapes=[
            space(nrhs, count), pltpu.VMEM(links.shape, jnp.int32), space(1, count), space(1, count),
            space(2, count), space(blocks, 2, count),
            space(leaders, SUB, count), space(blocks, SUB, count),
            space(leaders, SUB + 1, count), space(blocks, SUB + 1, count),
            space(count, count), space(2 * count, count), space(2, 2 * blocks, count),
            plane, plane, plane, plane, plane, plane, plane, plane, plane, plane,
            twice, plane, twice, space(SWEEPS * DEGREE, planes, SUB, count),
            space(SWEEPS, blocks, SUB, count),
            dma, dma, dma((2,)), dma((2,)), dma, dma,
        ],
        compiler_params=pltpu.CompilerParams(collective_id=0, has_side_effects=True),
    )(right_side, links, coefs.reshape(1, count), reaction.reshape(1, count))
    return pl.pallas_call(
        write_out,
        out_shape=(
            jax.ShapeDtypeStruct((nrhs, count), jnp.float32),
            jax.ShapeDtypeStruct((SWEEPS, nrhs), jnp.float32),
        ),
        in_specs=[vmem, vmem],
        out_specs=[pl.BlockSpec(memory_space=pl.ANY)] * 2,
        scratch_shapes=[dma((2,))],
    )(*[pltpu.with_memory_space_constraint(f, pltpu.VMEM) for f in found])


def in_one_kernel(mesh):
    return mesh.shape["grp"] == SUB // CX and 2 * SUB <= mesh.shape["row"] <= 4 * SUB


def solution(mesh):
    body = on_device
    if in_one_kernel(mesh):
        body = functools.partial(whole_sweeps, mesh.shape["grp"], mesh.shape["row"])
    return jax.shard_map(
        body,
        mesh=mesh,
        in_specs=(
            P(None, ("grp", "row")),
            P(None, ("grp", "row")),
            P(("grp", "row")),
            P(("grp", "row")),
        ),
        out_specs=(P(None, ("grp", "row")), P()),
        check_vma=False,
    )
```
